256 devices in a mesh: grp: 2 (over y), blk: 16 (over z), node: 4 (over x), pair: 2 (over core).
Axes of the slice: x: 4, y: 2, z: 16, core: 2. Of those that a mesh axis runs over, the one named last changes fastest.
The devices are a block of a 4x16x16 slice.
Arguments:
- query: bfloat16 [18432, 1280], P(('grp', 'blk', 'node'), 'pair'), parts along dimension 0, may hold values from -600 to 600
- key: bfloat16 [18432, 1280], P(('grp', 'blk', 'node'), 'pair'), parts along dimension 0, may hold values from -25 to 25
- value: bfloat16 [18432, 1280], P(('grp', 'blk', 'node'), 'pair'), parts along dimension 0, may hold values from -6 to 6
- out_weight: bfloat16 [1280, 1280], P('pair'), may hold values from -0.15625 to 0.15625
Outputs:
- mixed: bfloat16 [18432, 1280], P(('grp', 'blk', 'node', 'pair')), parts along dimension 0
The draws below stay inside these ranges and needn't reach their ends.
There are 2 independent parts, one for each index of `grp`. The reference program is written for one: setup_inputs(seed, part) draws one part's arguments, and reference() takes and returns one part's arrays. A program takes and returns all parts, laid end to end along the dimension named above; an argument that names none is the same for every part. Nothing has to cross between parts.
All inputs are finite; a program needn't handle non-finite values.
Results may differ from the reference program's by a relative error of at most 0.011.
Values may be sent and summed in bfloat16 or wider, within the bound.
A program may use at most 128 MiB of HBM per device.

```python
import math
import jax
import jax.numpy as jnp
from jax import lax

D = 1280
HEADS = 20
HD = 64
TOKENS = 9216


def key_rows(key):
    base = jnp.clip(jax.random.normal(jax.random.fold_in(key, 101), (TOKENS, D), jnp.float32), -4.5, 4.5)
    return base.astype(jnp.bfloat16)


def draw_key(key, part):
    return key_rows(key)


def draw_query(key, part):
    drawn = jax.random.normal(jax.random.fold_in(key, 105), (TOKENS, D), jnp.float32) * 2.5
    return jnp.clip(drawn, -12.0, 12.0).astype(jnp.bfloat16)


def block_levels(own_key, extent, shards, least, top_value):
    gain = 1.0
    for dim, shards_of in shards:
        steps = jax.random.uniform(jax.random.fold_in(jax.random.fold_in(own_key, 6), dim), (shards_of,), jnp.float32, least / len(shards), top_value / len(shards))
        gain = gain * jnp.repeat(jnp.exp(steps), extent[dim] // shards_of).reshape((-1,) + (1,) * (len(extent) - 1 - dim))
    return gain


def scatter_about(rng, shape, scale, reach, cuts=(), held_as=jnp.bfloat16):
    array = scale * jax.random.normal(rng, shape, jnp.float32)
    if cuts:
        array = array * block_levels(rng, shape, cuts, -0.22, 0.18)
    return jnp.clip(array, -reach, reach).astype(held_as)


def setup_inputs(seed: int = 0, part: int = 0) -> dict:
    keys = jax.random.split(jax.random.key(seed), 5)
    own_keys = jax.random.split(jax.random.fold_in(keys[4], part), 5)
    return {
        "query": draw_query(jax.random.fold_in(jax.random.fold_in(keys[4], part), 71), part),
        "key": draw_key(jax.random.fold_in(jax.random.fold_in(keys[4], part), 71), part),
        "value": scatter_about(own_keys[2], (TOKENS, D), 1.0, 6.0, ((0, 64), (1, 2))),
        "out_weight": scatter_about(keys[3], (D, D), D ** -0.5, 0.15625, ((0, 2),)),
    }


def reference(query, key, value, out_weight):
    scale = 1.0 / math.sqrt(HD)
    q_heads = query.reshape(TOKENS, HEADS, HD).transpose(1, 0, 2)
    k_heads = key.reshape(TOKENS, HEADS, HD).transpose(1, 0, 2)
    v_heads = value.reshape(TOKENS, HEADS, HD).transpose(1, 0, 2)

    def one_head(operands):
        q_one, k_one, v_one = operands
        scores = jnp.dot(q_one, k_one.T, preferred_element_type=jnp.float32) * scale
        peak = lax.optimization_barrier(jnp.max(scores, axis=1, keepdims=True))
        expo = jnp.exp(scores - peak)
        total = lax.optimization_barrier(jnp.sum(expo, axis=1, keepdims=True))
        return jnp.dot(expo.astype(jnp.bfloat16), v_one, preferred_element_type=jnp.float32) / total
    heads_out = lax.map(one_head, (q_heads, k_heads, v_heads))
    attn = heads_out.transpose(1, 0, 2).reshape(TOKENS, D).astype(jnp.bfloat16)
    return jnp.dot(attn, out_weight, preferred_element_type=jnp.float32).astype(jnp.bfloat16)
```

```python
import functools
import math

import jax
import jax.numpy as jnp
from jax import lax
from jax.experimental import pallas as pl
from jax.experimental.pallas import tpu as pltpu
from jax.sharding import PartitionSpec as P

HD = 64
LANES = 128
MESH = pl.DeviceIdType.MESH


def kernel(
    nz, nx, q_hbm, k_hbm, v_hbm, w_hbm, out_ref,
    kv, qall, qs, w, ml, acc, st_in, cb, cin, pacc, sbuf, rbuf,
    kv_send, kv_recv, q_send, q_recv, st_send, st_recv, c_send, c_recv, p_send, p_recv, loc,
):
    rows, features = q_hbm.shape
    pairs = features // LANES
    half = nz // 2
    nq = nx * rows
    z = lax.axis_index("blk")
    x = lax.axis_index("node")
    p = lax.axis_index("pair")
    z_next = (lax.rem(z + 1, nz), lax.rem(z + nz - 1, nz))
    scale2 = (1.0 / math.sqrt(HD)) * math.log2(math.e)

    def node(j):
        return lax.rem(x + j, nx)

    barrier = pltpu.get_barrier_semaphore()
    for d in range(2):
        pl.semaphore_signal(barrier, inc=1, device_id={"blk": z_next[d]}, device_id_type=MESH)
    for j in range(1, nx):
        pl.semaphore_signal(barrier, inc=1, device_id={"node": node(j)}, device_id_type=MESH)
    pl.semaphore_signal(barrier, inc=1, device_id={"pair": 1 - p}, device_id_type=MESH)

    def own_copy(r, part):
        src = (k_hbm, v_hbm)[part]
        return pltpu.make_async_copy(
            src.at[:, pl.ds(r * LANES, LANES)], kv.at[half, r, 0, part], loc.at[r, part]
        )

    for r in range(pairs):
        for part in range(2):
            own_copy(r, part).start()
    q_copy = pltpu.make_async_copy(q_hbm, qall.at[x], loc.at[pairs, 0])
    q_copy.start()
    w_copy = pltpu.make_async_copy(w_hbm, w, loc.at[pairs, 1])
    w_copy.start()
    pl.semaphore_wait(barrier, nx + 2)

    def full_msg(src, s, r, d):
        return pltpu.make_async_remote_copy(
            src_ref=src, dst_ref=kv.at[s, r, d],
            send_sem=kv_send.at[s - 1, r, d], recv_sem=kv_recv.at[s - 1, r, d],
            device_id={"blk": z_next[d]}, device_id_type=MESH,
        )

    def last_msg(src, r, d):
        return pltpu.make_async_remote_copy(
            src_ref=src, dst_ref=kv.at[half, r, 1, d],
            send_sem=kv_send.at[half - 1, r, d], recv_sem=kv_recv.at[half - 1, r, d],
            device_id={"blk": z_next[d]}, device_id_type=MESH,
        )

    def q_msg(j):
        return pltpu.make_async_remote_copy(
            src_ref=qall.at[x], dst_ref=qall.at[x],
            send_sem=q_send.at[j - 1], recv_sem=q_recv.at[j - 1],
            device_id={"node": node(j)}, device_id_type=MESH,
        )

    def q_arrival(j):
        return pltpu.make_async_remote_copy(
            src_ref=qall.at[node(nx - j)], dst_ref=qall.at[node(nx - j)],
            send_sem=q_send.at[j - 1], recv_sem=q_recv.at[j - 1],
            device_id={"node": node(j)}, device_id_type=MESH,
        )

    for r in range(pairs):
        own_copy(r, 0).wait()
        own_copy(r, 1).wait()
        for d in range(2):
            full_msg(kv.at[half, r, 0], 1, r, d).start()
    q_copy.wait()
    for j in range(1, nx):
        q_msg(j).start()

    ml[:, 0:1, :] = jnp.full((pairs, 1, 2 * nq), -1e30, jnp.float32)
    ml[:, 1:2, :] = jnp.zeros((pairs, 1, 2 * nq), jnp.float32)
    acc[...] = jnp.zeros(acc.shape, jnp.float32)

    def forward(t):
        s = t // pairs + 1
        r = lax.rem(t, pairs)
        for d in range(2):
            @pl.when(s < half)
            def _():
                full_msg(kv.at[half, r, 0], s, r, d).wait_recv()

            @pl.when(s == half)
            def _():
                last_msg(kv.at[half, r, 0, d], r, d).wait_recv()

            @pl.when(s < half - 1)
            def _():
                full_msg(kv.at[s, r, d], s + 1, r, d).start()

            @pl.when(s == half - 1)
            def _():
                last_msg(kv.at[s, r, d, d], r, d).start()

    width = 256

    def compute(t):
        s = t // pairs + 1
        r = lax.rem(t, pairs)
        keys = kv[s, r, :, 0].reshape(2 * rows, LANES)
        values = kv[s, r, :, 1].reshape(2 * rows, LANES)
        for lo in range(0, 2 * nq, width):
            hi = min(lo + width, 2 * nq)
            sc = lax.dot_general(
                keys, qs[r, lo:hi, :], (((1,), (1,)), ((), ())),
                preferred_element_type=jnp.float32,
            )
            old = ml[r, 0:1, lo:hi]
            new = jnp.maximum(old, jnp.max(sc, axis=0, keepdims=True))
            expo = jnp.exp2((sc - new) * scale2)
            factor = jnp.exp2((old - new) * scale2)
            ml[r, 0:1, lo:hi] = new
            ml[r, 1:2, lo:hi] = ml[r, 1:2, lo:hi] * factor + jnp.sum(expo, axis=0, keepdims=True)
            weighted = lax.dot_general(
                values, expo.astype(jnp.bfloat16), (((0,), (0,)), ((), ())),
                preferred_element_type=jnp.float32,
            )
            acc[r, :, lo:hi] = acc[r, :, lo:hi] * factor + weighted

    total = half * pairs

    @pl.loop(0, pairs)
    def _(t):
        forward(t)

    for j in range(1, nx):
        q_arrival(j).wait_recv()
    lane = lax.broadcasted_iota(jnp.int32, (rows, LANES), 1)
    for xa in range(nx):
        for r in range(pairs):
            block = qall[xa, :, r * LANES:(r + 1) * LANES].astype(jnp.float32)
            qs[r, xa * rows:(xa + 1) * rows, :] = jnp.where(lane < HD, block, 0.0).astype(jnp.bfloat16)
            qs[r, nq + xa * rows:nq + (xa + 1) * rows, :] = jnp.where(
                lane < HD, 0.0, block
            ).astype(jnp.bfloat16)

    def done_by(t):
        return jnp.where(t < pairs, 0, jnp.where(t < 2 * pairs - 1, t + 1 - pairs, t + 1))

    def st_msg(r, j):
        return pltpu.make_async_remote_copy(
            src_ref=ml.at[r], dst_ref=st_in.at[r, j - 1],
            send_sem=st_send.at[r, j - 1], recv_sem=st_recv.at[r, j - 1],
            device_id={"node": node(j)}, device_id_type=MESH,
        )

    def c_msg(r, j):
        return pltpu.make_async_remote_copy(
            src_ref=cb.at[r, node(j)], dst_ref=cin.at[r, j - 1],
            send_sem=c_send.at[r, j - 1], recv_sem=c_recv.at[r, j - 1],
            device_id={"node": node(j)}, device_id_type=MESH,
        )

    def spread(r):
        for j in range(1, nx):
            st_msg(r, j).wait_recv()
        best = ml[r, 0:1, :]
        for j in range(1, nx):
            best = jnp.maximum(best, st_in[r, j - 1, 0:1, :])
        mine = jnp.exp2((ml[r, 0:1, :] - best) * scale2)
        summed = ml[r, 1:2, :] * mine
        for j in range(1, nx):
            summed += st_in[r, j - 1, 1:2, :] * jnp.exp2((st_in[r, j - 1, 0:1, :] - best) * scale2)
        turned = (acc[r] * (mine / summed)).T
        lanes = lax.broadcasted_iota(jnp.int32, (nq, LANES), 1)
        both = jnp.where(lanes < HD, turned[:nq], turned[nq:]).astype(jnp.bfloat16)
        for xa in range(nx):
            cb[r, xa] = both[xa * rows:(xa + 1) * rows]
        for j in range(1, nx):
            c_msg(r, j).start()

    def project(r):
        for j in range(1, nx):
            c_msg(r, j).wait_recv()
        attn = cb[r, x].astype(jnp.float32)
        for j in range(1, nx):
            attn += cin[r, j - 1].astype(jnp.float32)
        pacc[...] += jnp.dot(
            attn.astype(jnp.bfloat16), w[pl.ds(r * LANES, LANES), :],
            preferred_element_type=jnp.float32,
        )

    @pl.loop(pairs, total)
    def _(t):
        forward(t)

        @pl.loop(done_by(t - 1), done_by(t))
        def _(c):
            compute(c)

        @pl.when(t >= total - pairs)
        def _():
            r = t - (total - pairs)
            for j in range(1, nx):
                st_msg(r, j).start()

    w_copy.wait()
    pacc[...] = jnp.zeros(pacc.shape, jnp.float32)

    @pl.loop(0, pairs)
    def _(r):
        spread(r)

    @pl.loop(0, pairs)
    def _(r):
        project(r)

    mine_rows = rows // 2
    sbuf[...] = pacc[pl.ds(pl.multiple_of((1 - p) * mine_rows, 8), mine_rows), :].astype(jnp.bfloat16)
    swap = pltpu.make_async_remote_copy(
        src_ref=sbuf, dst_ref=rbuf, send_sem=p_send, recv_sem=p_recv,
        device_id={"pair": 1 - p}, device_id_type=MESH,
    )
    swap.start()
    swap.wait_recv()
    out_ref[...] = (
        pacc[pl.ds(pl.multiple_of(p * mine_rows, 8), mine_rows), :] + rbuf[...].astype(jnp.float32)
    ).astype(out_ref.dtype)

    swap.wait_send()
    for j in range(1, nx):
        q_msg(j).wait_send()

    @pl.loop(0, pairs)
    def _(r):
        for j in range(1, nx):
            st_msg(r, j).wait_send()
            c_msg(r, j).wait_send()
        for d in range(2):
            last_msg(kv.at[half - 1, r, d, d], r, d).wait_send()

    @pl.loop(0, (half - 1) * pairs)
    def _(t):
        s = t // pairs + 1
        r = lax.rem(t, pairs)
        for d in range(2):
            full_msg(kv.at[half, r, 0], s, r, d).wait_send()


def solution(mesh):
    nz, nx = mesh.shape["blk"], mesh.shape["node"]
    half = nz // 2

    def per_device(query, key, value, out_weight):
        rows, features = query.shape
        pairs = features // LANES
        out_features = out_weight.shape[1]
        nq = nx * rows
        dma = pltpu.SemaphoreType.DMA
        any_space = pl.BlockSpec(memory_space=pl.ANY)
        bf16, f32 = jnp.bfloat16, jnp.float32
        return pl.pallas_call(
            functools.partial(kernel, nz, nx),
            out_shape=jax.ShapeDtypeStruct((rows // 2, out_features), bf16),
            in_specs=[any_space] * 4,
            out_specs=pl.BlockSpec(memory_space=pltpu.VMEM),
            scratch_shapes=[
                pltpu.VMEM((half + 1, pairs, 2, 2, rows, LANES), bf16),
                pltpu.VMEM((nx, rows, features), bf16),
                pltpu.VMEM((pairs, 2 * nq, LANES), bf16),
                pltpu.VMEM((features, out_features), bf16),
                pltpu.VMEM((pairs, 2, 2 * nq), f32),
                pltpu.VMEM((pairs, LANES, 2 * nq), f32),
                pltpu.VMEM((pairs, nx - 1, 2, 2 * nq), f32),
                pltpu.VMEM((pairs, nx, rows, LANES), bf16),
                pltpu.VMEM((pairs, nx - 1, rows, LANES), bf16),
                pltpu.VMEM((rows, out_features), f32),
                pltpu.VMEM((rows // 2, out_features), bf16),
                pltpu.VMEM((rows // 2, out_features), bf16),
                dma((half, pairs, 2)), dma((half, pairs, 2)),
                dma((nx - 1,)), dma((nx - 1,)),
                dma((pairs, nx - 1)), dma((pairs, nx - 1)),
                dma((pairs, nx - 1)), dma((pairs, nx - 1)),
                dma, dma, dma((pairs + 1, 2)),
            ],
            compiler_params=pltpu.CompilerParams(
                collective_id=0, has_side_effects=True, vmem_limit_bytes=48 * 1024 * 1024
            ),
        )(query, key, value, out_weight)

    tokens = P(("grp", "blk", "node"), "pair")
    return jax.shard_map(
        per_device,
        mesh=mesh,
        in_specs=(tokens, tokens, tokens, P("pair", None)),
        out_specs=P(("grp", "blk", "node", "pair"), None),
        check_vma=False,
    )
```

```python
import functools
import math

import jax
import jax.numpy as jnp
from jax import lax
from jax.experimental import pallas as pl
from jax.experimental.pallas import tpu as pltpu
from jax.sharding import PartitionSpec as P

HD = 64
LANES = 128
MESH = pl.DeviceIdType.MESH


def kernel(
    nz, nx, q_hbm, k_hbm, v_hbm, w_hbm, out_ref,
    kv, qall, qs, w, ml, acc, st_in, cb, cin, pacc, turned_w, sbuf, rbuf,
    kv_send, kv_recv, q_send, q_recv, st_send, st_recv, c_send, c_recv, p_send, p_recv, loc,
):
    rows, features = q_hbm.shape
    pairs = features // LANES
    half = nz // 2
    nq = nx * rows
    z = lax.axis_index("blk")
    x = lax.axis_index("node")
    p = lax.axis_index("pair")
    z_next = (lax.rem(z + 1, nz), lax.rem(z + nz - 1, nz))
    scale2 = (1.0 / math.sqrt(HD)) * math.log2(math.e)

    def node(j):
        return lax.rem(x + j, nx)

    barrier = pltpu.get_barrier_semaphore()
    for d in range(2):
        pl.semaphore_signal(barrier, inc=1, device_id={"blk": z_next[d]}, device_id_type=MESH)
    for j in range(1, nx):
        pl.semaphore_signal(barrier, inc=1, device_id={"node": node(j)}, device_id_type=MESH)
    pl.semaphore_signal(barrier, inc=1, device_id={"pair": 1 - p}, device_id_type=MESH)

    def own_copy(r, part):
        src = (k_hbm, v_hbm)[part]
        return pltpu.make_async_copy(
            src.at[:, pl.ds(r * LANES, LANES)], kv.at[half, r, 0, part], loc.at[r, part]
        )

    for r in range(pairs):
        for part in range(2):
            own_copy(r, part).start()
    q_copy = pltpu.make_async_copy(q_hbm, qall.at[x], loc.at[pairs, 0])
    q_copy.start()
    w_copy = pltpu.make_async_copy(w_hbm, w, loc.at[pairs, 1])
    w_copy.start()
    pl.semaphore_wait(barrier, nx + 2)

    def full_msg(src, s, r, d):
        return pltpu.make_async_remote_copy(
            src_ref=src, dst_ref=kv.at[s, r, d],
            send_sem=kv_send.at[s - 1, r, d], recv_sem=kv_recv.at[s - 1, r, d],
            device_id={"blk": z_next[d]}, device_id_type=MESH,
        )

    def last_msg(src, r, d):
        return pltpu.make_async_remote_copy(
            src_ref=src, dst_ref=kv.at[half, r, 1, d],
            send_sem=kv_send.at[half - 1, r, d], recv_sem=kv_recv.at[half - 1, r, d],
            device_id={"blk": z_next[d]}, device_id_type=MESH,
        )

    def q_msg(j):
        return pltpu.make_async_remote_copy(
            src_ref=qall.at[x], dst_ref=qall.at[x],
            send_sem=q_send.at[j - 1], recv_sem=q_recv.at[j - 1],
            device_id={"node": node(j)}, device_id_type=MESH,
        )

    def q_arrival(j):
        return pltpu.make_async_remote_copy(
            src_ref=qall.at[node(nx - j)], dst_ref=qall.at[node(nx - j)],
            send_sem=q_send.at[j - 1], recv_sem=q_recv.at[j - 1],
            device_id={"node": node(j)}, device_id_type=MESH,
        )

    for r in range(pairs):
        own_copy(r, 0).wait()
        own_copy(r, 1).wait()
        for d in range(2):
            full_msg(kv.at[half, r, 0], 1, r, d).start()
    q_copy.wait()
    for j in range(1, nx):
        q_msg(j).start()

    ml[:, 0:1, :] = jnp.full((pairs, 1, 2 * nq), -1e30, jnp.float32)
    ml[:, 1:2, :] = jnp.zeros((pairs, 1, 2 * nq), jnp.float32)
    acc[...] = jnp.zeros(acc.shape, jnp.float32)

    fast = 2
    slow = pairs - fast
    turn = fast + 1

    def unit(t):
        ahead = (t < turn * half) & (lax.rem(t, turn) < fast)
        k = jnp.where(t < turn * half, t // turn, t - fast * half)
        s = jnp.where(ahead, t // turn, k // slow) + 1
        r = jnp.where(ahead, lax.rem(t, turn), fast + lax.rem(k, slow))
        return s, r

    def forward(t):
        s, r = unit(t)
        for d in range(2):
            @pl.when(s < half)
            def _():
                full_msg(kv.at[half, r, 0], s, r, d).wait_recv()

            @pl.when(s == half)
            def _():
                last_msg(kv.at[half, r, 0, d], r, d).wait_recv()

            @pl.when(s < half - 1)
            def _():
                full_msg(kv.at[s, r, d], s + 1, r, d).start()

            @pl.when(s == half - 1)
            def _():
                last_msg(kv.at[s, r, d, d], r, d).start()

    width = 256

    def compute(t):
        s, r = unit(t)
        keys = kv[s, r, :, 0].reshape(2 * rows, LANES)
        values = kv[s, r, :, 1].reshape(2 * rows, LANES).T
        spans = [(lo, min(lo + width, 2 * nq)) for lo in range(0, 2 * nq, width)]

        def scored(span):
            lo, hi = span
            sc = lax.dot_general(
                keys, qs[r, lo:hi, :], (((1,), (1,)), ((), ())),
                preferred_element_type=jnp.float32,
            )
            old = ml[r, 0:1, lo:hi]
            return sc, old, jnp.maximum(old, jnp.max(sc, axis=0, keepdims=True))

        def weigh(span, sc, old, new):
            lo, hi = span
            expo = jnp.exp2((sc - new) * scale2)
            factor = jnp.exp2((old - new) * scale2)
            total_new = ml[r, 1:2, lo:hi] * factor + jnp.sum(expo, axis=0, keepdims=True)
            top = HD if lo >= nq else 0
            end = HD if hi <= nq else LANES
            weighted = jnp.dot(
                values[top:end], expo.astype(jnp.bfloat16), preferred_element_type=jnp.float32
            )
            return new, total_new, factor, weighted, top, end

        ready = scored(spans[0])
        results = []
        for i, span in enumerate(spans):
            following = scored(spans[i + 1]) if i + 1 < len(spans) else None
            results.append(weigh(span, *ready))
            ready = following
        for (lo, hi), (new, total_new, factor, weighted, top, end) in zip(spans, results):
            ml[r, 0:1, lo:hi] = new
            ml[r, 1:2, lo:hi] = total_new
            acc[r, top:end, lo:hi] = acc[r, top:end, lo:hi] * factor + weighted

    total = half * pairs

    before_q = min(6, (turn * (half - 1) + 1) // 2)

    @pl.loop(0, before_q)
    def _(t):
        forward(t)

    for j in range(1, nx):
        q_arrival(j).wait_recv()
    lane = lax.broadcasted_iota(jnp.int32, (rows, LANES), 1)
    for xa in range(nx):
        for r in range(pairs):
            block = qall[xa, :, r * LANES:(r + 1) * LANES].astype(jnp.float32)
            qs[r, xa * rows:(xa + 1) * rows, :] = jnp.where(lane < HD, block, 0.0).astype(jnp.bfloat16)
            qs[r, nq + xa * rows:nq + (xa + 1) * rows, :] = jnp.where(
                lane < HD, 0.0, block
            ).astype(jnp.bfloat16)

    def done_by(t):
        return jnp.clip(2 * (t - before_q + 1), 0, t + 1)

    def st_msg(r, j):
        return pltpu.make_async_remote_copy(
            src_ref=ml.at[r], dst_ref=st_in.at[r, j - 1],
            send_sem=st_send.at[r, j - 1], recv_sem=st_recv.at[r, j - 1],
            device_id={"node": node(j)}, device_id_type=MESH,
        )

    def c_msg(r, j):
        return pltpu.make_async_remote_copy(
            src_ref=cb.at[r, node(j)], dst_ref=cin.at[r, j - 1],
            send_sem=c_send.at[r, j - 1], recv_sem=c_recv.at[r, j - 1],
            device_id={"node": node(j)}, device_id_type=MESH,
        )

    def spread(r):
        for j in range(1, nx):
            st_msg(r, j).start()
        turned = (acc[r] * (1.0 / ml[r, 1:2, :])).T
        lanes = lax.broadcasted_iota(jnp.int32, (nq, LANES), 1)
        both = jnp.where(lanes < HD, turned[:nq], turned[nq:]).astype(jnp.bfloat16)
        for xa in range(nx):
            cb[r, xa] = both[xa * rows:(xa + 1) * rows]
        for j in range(1, nx):
            c_msg(r, j).start()

    def project(r):
        for j in range(1, nx):
            st_msg(r, j).wait_recv()
        stats = [ml.at[r]] + [st_in.at[r, j - 1] for j in range(1, nx)]
        best = functools.reduce(jnp.maximum, [st[0:1, :] for st in stats])
        shares = [jnp.exp2((st[0:1, :] - best) * scale2) * st[1:2, :] for st in stats]
        inverse = 1.0 / sum(shares)
        blank = jnp.zeros((LANES - nx, 2 * nq), jnp.float32)
        turned_w[...] = jnp.concatenate([share * inverse for share in shares] + [blank], axis=0).T
        mine_a = turned_w[pl.ds(pl.multiple_of(x * rows, 8), rows), :]
        mine_b = turned_w[pl.ds(pl.multiple_of(nq + x * rows, 8), rows), :]
        attn = jnp.zeros((rows, LANES), jnp.float32)
        for j in range(nx):
            if j:
                c_msg(r, j).wait_recv()
            part = cin[r, j - 1] if j else cb[r, x]
            share = jnp.where(lane < HD, mine_a[:, j:j + 1], mine_b[:, j:j + 1])
            attn += share * part.astype(jnp.float32)
        pacc[...] += jnp.dot(
            attn.astype(jnp.bfloat16), w[pl.ds(r * LANES, LANES), :],
            preferred_element_type=jnp.float32,
        )

    @pl.loop(before_q, total)
    def _(t):
        forward(t)

        @pl.loop(done_by(t - 1), done_by(t))
        def _(c):
            compute(c)

        s, r = unit(t)

        @pl.when(s == half)
        def _():
            spread(r)

    w_copy.wait()
    pacc[...] = jnp.zeros(pacc.shape, jnp.float32)

    @pl.loop(0, pairs)
    def _(r):
        project(r)

    mine_rows = rows // 2
    sbuf[...] = pacc[pl.ds(pl.multiple_of((1 - p) * mine_rows, 8), mine_rows), :].astype(jnp.bfloat16)
    swap = pltpu.make_async_remote_copy(
        src_ref=sbuf, dst_ref=rbuf, send_sem=p_send, recv_sem=p_recv,
        device_id={"pair": 1 - p}, device_id_type=MESH,
    )
    swap.start()
    swap.wait_recv()
    out_ref[...] = (
        pacc[pl.ds(pl.multiple_of(p * mine_rows, 8), mine_rows), :] + rbuf[...].astype(jnp.float32)
    ).astype(out_ref.dtype)

    swap.wait_send()
    for j in range(1, nx):
        q_msg(j).wait_send()

    @pl.loop(0, pairs)
    def _(r):
        for j in range(1, nx):
            st_msg(r, j).wait_send()
            c_msg(r, j).wait_send()
        for d in range(2):
            last_msg(kv.at[half - 1, r, d, d], r, d).wait_send()

    @pl.loop(0, (half - 1) * pairs)
    def _(t):
        s = t // pairs + 1
        r = lax.rem(t, pairs)
        for d in range(2):
            full_msg(kv.at[half, r, 0], s, r, d).wait_send()


def solution(mesh):
    nz, nx = mesh.shape["blk"], mesh.shape["node"]
    half = nz // 2

    def per_device(query, key, value, out_weight):
        rows, features = query.shape
        pairs = features // LANES
        out_features = out_weight.shape[1]
        nq = nx * rows
        dma = pltpu.SemaphoreType.DMA
        any_space = pl.BlockSpec(memory_space=pltpu.HBM)
        bf16, f32 = jnp.bfloat16, jnp.float32
        return pl.pallas_call(
            functools.partial(kernel, nz, nx),
            out_shape=jax.ShapeDtypeStruct((rows // 2, out_features), bf16),
            in_specs=[any_space] * 4,
            out_specs=pl.BlockSpec(memory_space=pltpu.VMEM),
            scratch_shapes=[
                pltpu.VMEM((half + 1, pairs, 2, 2, rows, LANES), bf16),
                pltpu.VMEM((nx, rows, features), bf16),
                pltpu.VMEM((pairs, 2 * nq, LANES), bf16),
                pltpu.VMEM((features, out_features), bf16),
                pltpu.VMEM((pairs, 2, 2 * nq), f32),
                pltpu.VMEM((pairs, LANES, 2 * nq), f32),
                pltpu.VMEM((pairs, nx - 1, 2, 2 * nq), f32),
                pltpu.VMEM((pairs, nx, rows, LANES), bf16),
                pltpu.VMEM((pairs, nx - 1, rows, LANES), bf16),
                pltpu.VMEM((rows, out_features), f32),
                pltpu.VMEM((2 * nq, LANES), f32),
                pltpu.VMEM((rows // 2, out_features), bf16),
                pltpu.VMEM((rows // 2, out_features), bf16),
                dma((half, pairs, 2)), dma((half, pairs, 2)),
                dma((nx - 1,)), dma((nx - 1,)),
                dma((pairs, nx - 1)), dma((pairs, nx - 1)),
                dma((pairs, nx - 1)), dma((pairs, nx - 1)),
                dma, dma, dma((pairs + 1, 2)),
            ],
            compiler_params=pltpu.CompilerParams(
                collective_id=0, has_side_effects=True, vmem_limit_bytes=67043328 - 256 * 1024
            ),
        )(query, key, value, out_weight)

    tokens = P(("grp", "blk", "node"), "pair")
    return jax.shard_map(
        per_device,
        mesh=mesh,
        in_specs=(tokens, tokens, tokens, P("pair", None)),
        out_specs=P(("grp", "blk", "node", "pair"), None),
        check_vma=False,
    )
```

```python
import functools
import math

import jax
import jax.numpy as jnp
from jax import lax
from jax.experimental import pallas as pl
from jax.experimental.pallas import tpu as pltpu
from jax.sharding import PartitionSpec as P

HD = 64
LANES = 128
GROUP = 4
MESH = pl.DeviceIdType.MESH


def up(n, m):
    return -(-n // m) * m


def kernel(
    nz, nx, near, q_hbm, k_hbm, v_hbm, w_hbm, out_ref,
    q_in, k_in, v_in, w, kvp, qp, kvb, qin, qrows, ml, acc, turned, ob, oin, attn, sbuf, rbuf,
    z_send, z_recv, q_send, q_recv, x_send, x_recv, d_send, d_recv, o_send, o_recv,
    p_send, p_recv, loc, own_sem,
):
    rows, features = q_hbm.shape
    heads = features // HD
    tiles = features // LANES
    half_rows = rows // 2
    half = nz // 2
    z = lax.axis_index("blk")
    x = lax.axis_index("node")
    p = lax.axis_index("pair")
    scale2 = (1.0 / math.sqrt(HD)) * math.log2(math.e)
    offsets = [0]
    for d in range(1, half):
        offsets += [d, -d]
    offsets.append(half)
    shared = [d for d in offsets if d % GROUP == 0]
    far = nz - near
    messages = near
    side = lax.div(z, half)
    in_side = z - side * half
    lead = lax.div(in_side, GROUP) * (GROUP + 1)
    head_own = lead + lax.rem(in_side, GROUP)
    head_shared = lead + GROUP
    split = up(far * rows, LANES)
    nq = ml.shape[1]

    def plane(d):
        return lax.rem(z + nz + d, nz)

    def node(j):
        return lax.rem(x + j, nx)

    barrier = pltpu.get_barrier_semaphore()
    for d in offsets[1:]:
        for c in range(2):
            pl.semaphore_signal(
                barrier, inc=1, device_id={"blk": plane(d), "pair": c}, device_id_type=MESH
            )
    for j in range(1, nx):
        pl.semaphore_signal(barrier, inc=1, device_id={"node": node(j)}, device_id_type=MESH)
    pl.semaphore_signal(barrier, inc=1, device_id={"pair": 1 - p}, device_id_type=MESH)

    loads = [
        pltpu.make_async_copy(src, dst, loc.at[i])
        for i, (src, dst) in enumerate(((q_hbm, q_in), (k_hbm, k_in), (v_hbm, v_in), (w_hbm, w)))
    ]
    for load in loads:
        load.start()

    low = lax.broadcasted_iota(jnp.int32, (rows, LANES), 1) < HD
    low_half = lax.broadcasted_iota(jnp.int32, (half_rows, LANES), 1) < HD

    def swap_sides(a):
        return pltpu.roll(a, HD, 1)

    loads[0].wait()
    for i in range(tiles):
        tile = q_in[:, i * LANES:(i + 1) * LANES].astype(jnp.float32)
        top, bottom = tile[:half_rows], tile[half_rows:]
        qp[2 * i] = jnp.where(low_half, top, swap_sides(bottom)).astype(jnp.bfloat16)
        qp[2 * i + 1] = jnp.where(low_half, swap_sides(top), bottom).astype(jnp.bfloat16)
    loads[1].wait()
    loads[2].wait()
    for i in range(tiles):
        k_tile = k_in[:, i * LANES:(i + 1) * LANES].astype(jnp.float32)
        v_tile = v_in[:, i * LANES:(i + 1) * LANES].astype(jnp.float32)
        kvp[2 * i] = jnp.where(low, k_tile, swap_sides(v_tile)).astype(jnp.bfloat16)
        kvp[2 * i + 1] = jnp.where(low, swap_sides(k_tile), v_tile).astype(jnp.bfloat16)
    ml[0:1, :] = jnp.full((1, nq), -1e30, jnp.float32)
    ml[1:2, :] = jnp.zeros((1, nq), jnp.float32)
    acc[...] = jnp.zeros(acc.shape, jnp.float32)
    qrows[...] = jnp.zeros(qrows.shape, jnp.bfloat16)

    def full_place(d):
        i = offsets.index(d)
        return (0, i) if i < near else (1, i - near)

    def shared_place(d):
        return 1, far + shared.index(d)

    def opposite(e):
        return half if e == half else -e

    def target_heads(zt):
        first = lax.div(zt - p * half, GROUP) * (GROUP + 1)
        return first + lax.rem(zt, GROUP), first + GROUP

    def kv_msg(e, kind):
        slot = offsets.index(opposite(e))
        zt = plane(e)
        return pltpu.make_async_remote_copy(
            src_ref=kvp.at[target_heads(zt)[kind]], dst_ref=kvb.at[0, slot, x],
            send_sem=z_send.at[slot, kind], recv_sem=z_recv.at[slot],
            device_id={"blk": zt, "pair": kind}, device_id_type=MESH,
        )

    def q_msg(e, kind):
        zt = plane(e)
        core, place = (full_place, shared_place)[kind](opposite(e))
        return pltpu.make_async_remote_copy(
            src_ref=qp.at[target_heads(zt)[kind]], dst_ref=qin.at[place],
            send_sem=q_send.at[offsets.index(e), kind], recv_sem=q_recv.at[place],
            device_id={"blk": zt, "pair": core}, device_id_type=MESH,
        )

    def mine(e):
        return lax.div(plane(e), half) == p

    def own_kv_local():
        return pltpu.make_async_copy(
            kvp.at[jnp.where(p == 0, head_own, head_shared)], kvb.at[0, 0, x], own_sem.at[0]
        )

    def own_kv_msg():
        return pltpu.make_async_remote_copy(
            src_ref=kvp.at[jnp.where(p == 0, head_shared, head_own)], dst_ref=kvb.at[0, 0, x],
            send_sem=z_send.at[0, 0], recv_sem=z_recv.at[0],
            device_id={"pair": 1 - p}, device_id_type=MESH,
        )

    def own_q_local():
        return pltpu.make_async_copy(
            qp.at[jnp.where(p == 0, head_own, head_shared)],
            qin.at[jnp.where(p == 0, 0, far)], own_sem.at[1],
        )

    def own_q_msg():
        there = jnp.where(p == 0, far, 0)
        return pltpu.make_async_remote_copy(
            src_ref=qp.at[jnp.where(p == 0, head_shared, head_own)], dst_ref=qin.at[there],
            send_sem=q_send.at[0, 0], recv_sem=q_recv.at[there],
            device_id={"pair": 1 - p}, device_id_type=MESH,
        )

    pl.semaphore_wait(barrier, 2 * (nz - 1) + nx)

    @pl.when(side == p)
    def _():
        own_q_local().start()
        own_kv_local().start()
        own_q_msg().start()
        own_kv_msg().start()

    for e in offsets[1:]:
        @pl.when(mine(e))
        def _():
            q_msg(e, 0).start()
            if e % GROUP == 0:
                q_msg(e, 1).start()
    for e in offsets[1:]:
        @pl.when(mine(e))
        def _():
            kv_msg(e, 0).start()
            kv_msg(e, 1).start()

    def x_msg(i, j):
        return pltpu.make_async_remote_copy(
            src_ref=kvb.at[0, i, x], dst_ref=kvb.at[0, i, x],
            send_sem=x_send.at[i, j - 1], recv_sem=x_recv.at[i, j - 1],
            device_id={"node": node(j)}, device_id_type=MESH,
        )

    def across(i, j):
        col = node(nx - j)
        return pltpu.make_async_remote_copy(
            src_ref=kvb.at[0, i, col], dst_ref=kvb.at[1, i, col],
            send_sem=d_send.at[i, j], recv_sem=d_recv.at[i, j],
            device_id={"pair": 1 - p}, device_id_type=MESH,
        )

    def arrive(i):
        @pl.when((i == 0) & (side == p))
        def _():
            own_kv_local().wait()

        @pl.when((i > 0) | (side != p))
        def _():
            pltpu.make_async_remote_copy(
                src_ref=kvb.at[0, i, x], dst_ref=kvb.at[0, i, x],
                send_sem=z_send.at[0, 0], recv_sem=z_recv.at[i],
                device_id={"pair": 1 - p}, device_id_type=MESH,
            ).wait_recv()

        for j in range(1, nx):
            x_msg(i, j).start()

        @pl.when(p == 0)
        def _():
            across(i, 0).start()

    def spread(i):
        for j in range(1, nx):
            col = node(nx - j)
            pltpu.make_async_remote_copy(
                src_ref=kvb.at[0, i, col], dst_ref=kvb.at[0, i, col],
                send_sem=x_send.at[i, j - 1], recv_sem=x_recv.at[i, j - 1],
                device_id={"node": node(j)}, device_id_type=MESH,
            ).wait_recv()

            @pl.when(p == 0)
            def _():
                across(i, j).start()

    width = 256
    spans = [(lo, min(lo + width, split), 1) for lo in range(0, split, width)]
    spans += [(hi, min(lo, nq), 0) for hi, lo in (
        [(split, up(split + 1, width))] + [(lo, lo + width) for lo in range(up(split + 1, width), nq, width)]
    ) if hi < nq]

    def compute(i):
        @pl.when(p == 1)
        def _():
            for j in range(nx):
                across(i, j).wait_recv()

        first = kvb[p, i].reshape(nx * rows, LANES)
        second = kvb[0, i].reshape(nx * rows, LANES)
        keys = (second, first)
        values = (second.T[HD:], first.T[HD:])

        def scored(span):
            lo, hi, kind = span
            sc = lax.dot_general(
                keys[kind], qrows[lo:hi, :], (((1,), (1,)), ((), ())),
                preferred_element_type=jnp.float32,
            )
            old = ml[0:1, lo:hi]
            return sc, old, jnp.maximum(old, jnp.max(sc, axis=0, keepdims=True))

        def weigh(span, sc, old, new):
            lo, hi, kind = span
            expo = jnp.exp2((sc - new) * scale2)
            factor = jnp.exp2((old - new) * scale2)
            total = ml[1:2, lo:hi] * factor + jnp.sum(expo, axis=0, keepdims=True)
            weighted = jnp.dot(
                values[kind], expo.astype(jnp.bfloat16), preferred_element_type=jnp.float32
            )
            return new, total, factor, weighted

        ready = scored(spans[0])
        results = []
        for n, span in enumerate(spans):
            following = scored(spans[n + 1]) if n + 1 < len(spans) else None
            results.append(weigh(span, *ready))
            ready = following
        for (lo, hi, _), (new, total, factor, weighted) in zip(spans, results):
            ml[0:1, lo:hi] = new
            ml[1:2, lo:hi] = total
            acc[:, lo:hi] = acc[:, lo:hi] * factor + weighted

    arrive(0)
    arrive(1)
    spread(0)

    def base(a):
        return pl.multiple_of(a * rows + jnp.where((p == 1) & (a >= far), split - far * rows, 0), 16)

    @pl.loop(0, messages)
    def _(a):
        own = (side == p) & (a == jnp.where(p == 0, 0, far))

        @pl.when(own)
        def _():
            own_q_local().wait()

        @pl.when(jnp.logical_not(own))
        def _():
            pltpu.make_async_remote_copy(
                src_ref=qin.at[a], dst_ref=qin.at[a], send_sem=q_send.at[0, 0],
                recv_sem=q_recv.at[a], device_id={"pair": 1 - p}, device_id_type=MESH,
            ).wait_recv()

        block = qin[a].astype(jnp.float32)
        both = jnp.concatenate(
            [jnp.where(low_half, block, 0.0), jnp.where(low_half, swap_sides(block), 0.0)], axis=0
        )
        qrows[pl.ds(base(a), rows), :] = both.astype(jnp.bfloat16)

    @pl.loop(0, nz)
    def _(i):
        @pl.when(i + 2 < nz)
        def _():
            arrive(i + 2)

        @pl.when(i + 1 < nz)
        def _():
            spread(i + 1)

        compute(i)

    def back(a):
        d = jnp.where(p == 0, offsets[a], (offsets[near:] + shared)[a])
        h = jnp.where((p == 1) & (a >= far), head_shared, head_own)
        return d, h

    def o_local(a):
        return pltpu.make_async_copy(ob.at[a], oin.at[back(a)[1]], own_sem.at[2])

    def o_msg(a):
        d, h = back(a)
        return pltpu.make_async_remote_copy(
            src_ref=ob.at[a], dst_ref=oin.at[h], send_sem=o_send.at[a], recv_sem=o_recv.at[h],
            device_id={"blk": plane(d), "pair": side}, device_id_type=MESH,
        )

    blank = jnp.zeros((LANES - HD, nq), jnp.float32)
    turned[...] = jnp.concatenate([acc[...] * (1.0 / ml[1:2, :]), blank], axis=0).T
    for a in range(messages):
        block = turned[pl.ds(base(a), rows), :]
        ob[a] = (block[:half_rows] + swap_sides(block[half_rows:])).astype(jnp.bfloat16)
        here = (back(a)[0] == 0) & (side == p)

        @pl.when(here)
        def _():
            o_local(a).start()

        @pl.when(jnp.logical_not(here))
        def _():
            o_msg(a).start()

    loads[3].wait()
    for i in range(tiles):
        for h in (2 * i, 2 * i + 1):
            g, n = divmod(h, GROUP + 1)
            zt = p * half + g * GROUP + (n if n < GROUP else lax.rem(z, GROUP))
            here = (zt == z) & (p == (0 if n < GROUP else 1))

            @pl.when(here)
            def _():
                pltpu.make_async_copy(ob.at[0], oin.at[h], own_sem.at[2]).wait()

            @pl.when(jnp.logical_not(here))
            def _():
                pltpu.make_async_remote_copy(
                    src_ref=oin.at[h], dst_ref=oin.at[h], send_sem=o_send.at[0],
                    recv_sem=o_recv.at[h], device_id={"pair": 1 - p}, device_id_type=MESH,
                ).wait_recv()

        even = oin[2 * i].astype(jnp.float32)
        odd = oin[2 * i + 1].astype(jnp.float32)
        cols = slice(i * LANES, (i + 1) * LANES)
        attn[0, :, cols] = jnp.where(low_half, even, swap_sides(odd)).astype(jnp.bfloat16)
        attn[1, :, cols] = jnp.where(low_half, swap_sides(even), odd).astype(jnp.bfloat16)

    sbuf[...] = jnp.dot(attn[1 - p], w[...], preferred_element_type=jnp.float32).astype(jnp.bfloat16)
    swap = pltpu.make_async_remote_copy(
        src_ref=sbuf, dst_ref=rbuf, send_sem=p_send, recv_sem=p_recv,
        device_id={"pair": 1 - p}, device_id_type=MESH,
    )
    swap.start()
    kept = jnp.dot(attn[p], w[...], preferred_element_type=jnp.float32)
    swap.wait_recv()
    out_ref[...] = (kept + rbuf[...].astype(jnp.float32)).astype(out_ref.dtype)
    swap.wait_send()

    @pl.when(side == p)
    def _():
        own_q_msg().wait_send()
        own_kv_msg().wait_send()

    for e in offsets[1:]:
        @pl.when(mine(e))
        def _():
            q_msg(e, 0).wait_send()
            if e % GROUP == 0:
                q_msg(e, 1).wait_send()
            kv_msg(e, 0).wait_send()
            kv_msg(e, 1).wait_send()

    @pl.loop(0, nz)
    def _(i):
        for j in range(1, nx):
            x_msg(i, j).wait_send()

        @pl.when(p == 0)
        def _():
            for j in range(nx):
                across(i, j).wait_send()

    for a in range(messages):
        @pl.when(jnp.logical_not((back(a)[0] == 0) & (side == p)))
        def _():
            o_msg(a).wait_send()


def solution(mesh):
    nz, nx = mesh.shape["blk"], mesh.shape["node"]

    def per_device(query, key, value, out_weight):
        rows, features = query.shape
        heads = features // HD
        assert nz % (2 * GROUP) == 0 and heads == nz // 2 // GROUP * (GROUP + 1)
        near = heads
        far = nz - near
        split = up(far * rows, LANES)
        nq = max(up(near * rows, LANES), split + up((nz // GROUP) * rows, LANES))
        out_features = out_weight.shape[1]
        dma = pltpu.SemaphoreType.DMA
        any_space = pl.BlockSpec(memory_space=pltpu.HBM)
        bf16, f32 = jnp.bfloat16, jnp.float32
        return pl.pallas_call(
            functools.partial(kernel, nz, nx, near),
            out_shape=jax.ShapeDtypeStruct((rows // 2, out_features), bf16),
            in_specs=[any_space] * 4,
            out_specs=pl.BlockSpec(memory_space=pltpu.VMEM),
            scratch_shapes=[
                pltpu.VMEM((rows, features), bf16),
                pltpu.VMEM((rows, features), bf16),
                pltpu.VMEM((rows, features), bf16),
                pltpu.VMEM((features, out_features), bf16),
                pltpu.VMEM((heads, rows, LANES), bf16),
                pltpu.VMEM((heads, rows // 2, LANES), bf16),
                pltpu.VMEM((2, nz, nx, rows, LANES), bf16),
                pltpu.VMEM((near, rows // 2, LANES), bf16),
                pltpu.VMEM((nq, LANES), bf16),
                pltpu.VMEM((2, nq), f32),
                pltpu.VMEM((HD, nq), f32),
                pltpu.VMEM((nq, LANES), f32),
                pltpu.VMEM((near, rows // 2, LANES), bf16),
                pltpu.VMEM((heads, rows // 2, LANES), bf16),
                pltpu.VMEM((2, rows // 2, features), bf16),
                pltpu.VMEM((rows // 2, out_features), bf16),
                pltpu.VMEM((rows // 2, out_features), bf16),
                dma((nz, 2)), dma((nz,)), dma((nz, 2)), dma((near,)),
                dma((nz, nx - 1)), dma((nz, nx - 1)), dma((nz, nx)), dma((nz, nx)),
                dma((near,)), dma((heads,)), dma, dma, dma((4,)), dma((3,)),
            ],
            compiler_params=pltpu.CompilerParams(
                collective_id=0, has_side_effects=True, vmem_limit_bytes=67043328 - 256 * 1024
            ),
        )(query, key, value, out_weight)

    tokens = P(("grp", "blk", "node"), "pair")
    return jax.shard_map(
        per_device,
        mesh=mesh,
        in_specs=(tokens, tokens, tokens, P("pair", None)),
        out_specs=P(("grp", "blk", "node", "pair"), None),
        check_vma=False,
    )
```

```python
import functools
import math

import jax
import jax.numpy as jnp
from jax import lax
from jax.experimental import pallas as pl
from jax.experimental.pallas import tpu as pltpu
from jax.sharding import PartitionSpec as P

HD = 64
LANES = 128
GROUP = 4
MESH = pl.DeviceIdType.MESH


def up(n, m):
    return -(-n // m) * m


def kernel(
    nz, nx, near, q_hbm, k_hbm, v_hbm, w_hbm, out_ref,
    q_in, k_in, v_in, w, kvp, qp, kvb, qin, qrows, ml, acc, turned, ob, oin, attn, sbuf, rbuf,
    z_send, z_recv, q_send, q_recv, x_send, x_recv, d_send, d_recv, o_send, o_recv,
    p_send, p_recv, loc, own_sem,
):
    rows, features = q_hbm.shape
    heads = features // HD
    tiles = features // LANES
    half_rows = rows // 2
    half = nz // 2
    z = lax.axis_index("blk")
    x = lax.axis_index("node")
    p = lax.axis_index("pair")
    scale2 = (1.0 / math.sqrt(HD)) * math.log2(math.e)
    offsets = [0]
    for d in range(1, half):
        offsets += [d, -d]
    offsets.append(half)
    shared = [d for d in offsets if d % GROUP == 0]
    far = nz - near
    messages = near
    side = lax.div(z, half)
    in_side = z - side * half
    lead = lax.div(in_side, GROUP) * (GROUP + 1)
    head_own = lead + lax.rem(in_side, GROUP)
    head_shared = lead + GROUP
    split = up(far * rows, LANES)
    nq = ml.shape[1]

    def plane(d):
        return lax.rem(z + nz + d, nz)

    def node(j):
        return lax.rem(x + j, nx)

    barrier = pltpu.get_barrier_semaphore()
    for d in offsets[1:]:
        for c in range(2):
            pl.semaphore_signal(
                barrier, inc=1, device_id={"blk": plane(d), "pair": c}, device_id_type=MESH
            )
    for j in range(1, nx):
        pl.semaphore_signal(barrier, inc=1, device_id={"node": node(j)}, device_id_type=MESH)
    pl.semaphore_signal(barrier, inc=1, device_id={"pair": 1 - p}, device_id_type=MESH)

    loads = [
        pltpu.make_async_copy(src, dst, loc.at[i])
        for i, (src, dst) in enumerate(((q_hbm, q_in), (k_hbm, k_in), (v_hbm, v_in), (w_hbm, w)))
    ]
    for load in loads:
        load.start()

    low = lax.broadcasted_iota(jnp.int32, (rows, LANES), 1) < HD
    low_half = lax.broadcasted_iota(jnp.int32, (half_rows, LANES), 1) < HD

    def swap_sides(a):
        return pltpu.roll(a, HD, 1)

    loads[0].wait()
    for i in range(tiles):
        tile = q_in[:, i * LANES:(i + 1) * LANES].astype(jnp.float32)
        top, bottom = tile[:half_rows], tile[half_rows:]
        qp[2 * i] = jnp.where(low_half, top, swap_sides(bottom)).astype(jnp.bfloat16)
        qp[2 * i + 1] = jnp.where(low_half, swap_sides(top), bottom).astype(jnp.bfloat16)
    loads[1].wait()
    loads[2].wait()
    for i in range(tiles):
        k_tile = k_in[:, i * LANES:(i + 1) * LANES].astype(jnp.float32)
        v_tile = v_in[:, i * LANES:(i + 1) * LANES].astype(jnp.float32)
        kvp[2 * i] = jnp.where(low, k_tile, swap_sides(v_tile)).astype(jnp.bfloat16)
        kvp[2 * i + 1] = jnp.where(low, swap_sides(k_tile), v_tile).astype(jnp.bfloat16)
    ml[0:1, :] = jnp.full((1, nq), -1e30, jnp.float32)
    ml[1:2, :] = jnp.zeros((1, nq), jnp.float32)
    acc[...] = jnp.zeros(acc.shape, jnp.float32)
    qrows[...] = jnp.zeros(qrows.shape, jnp.bfloat16)

    def full_place(d):
        i = offsets.index(d)
        return (0, i) if i < near else (1, i - near)

    def shared_place(d):
        return 1, far + shared.index(d)

    def opposite(e):
        return half if e == half else -e

    def target_heads(zt):
        first = lax.div(zt - p * half, GROUP) * (GROUP + 1)
        return first + lax.rem(zt, GROUP), first + GROUP

    def kv_msg(e, kind):
        slot = offsets.index(opposite(e))
        zt = plane(e)
        return pltpu.make_async_remote_copy(
            src_ref=kvp.at[target_heads(zt)[kind]], dst_ref=kvb.at[0, slot, x],
            send_sem=z_send.at[slot, kind], recv_sem=z_recv.at[slot],
            device_id={"blk": zt, "pair": kind}, device_id_type=MESH,
        )

    def q_msg(e, kind):
        zt = plane(e)
        core, place = (full_place, shared_place)[kind](opposite(e))
        return pltpu.make_async_remote_copy(
            src_ref=qp.at[target_heads(zt)[kind]], dst_ref=qin.at[place],
            send_sem=q_send.at[offsets.index(e), kind], recv_sem=q_recv.at[place],
            device_id={"blk": zt, "pair": core}, device_id_type=MESH,
        )

    def mine(e):
        return lax.div(plane(e), half) == p

    def own_kv_local():
        return pltpu.make_async_copy(
            kvp.at[jnp.where(p == 0, head_own, head_shared)], kvb.at[0, 0, x], own_sem.at[0]
        )

    def own_kv_msg():
        return pltpu.make_async_remote_copy(
            src_ref=kvp.at[jnp.where(p == 0, head_shared, head_own)], dst_ref=kvb.at[0, 0, x],
            send_sem=z_send.at[0, 0], recv_sem=z_recv.at[0],
            device_id={"pair": 1 - p}, device_id_type=MESH,
        )

    def own_q_local():
        return pltpu.make_async_copy(
            qp.at[jnp.where(p == 0, head_own, head_shared)],
            qin.at[jnp.where(p == 0, 0, far)], own_sem.at[1],
        )

    def own_q_msg():
        there = jnp.where(p == 0, far, 0)
        return pltpu.make_async_remote_copy(
            src_ref=qp.at[jnp.where(p == 0, head_shared, head_own)], dst_ref=qin.at[there],
            send_sem=q_send.at[0, 0], recv_sem=q_recv.at[there],
            device_id={"pair": 1 - p}, device_id_type=MESH,
        )

    pl.semaphore_wait(barrier, 2 * (nz - 1) + nx)

    @pl.when(side == p)
    def _():
        own_q_local().start()
        own_kv_local().start()
        own_q_msg().start()
        own_kv_msg().start()

    for e in offsets[1:]:
        @pl.when(mine(e))
        def _():
            q_msg(e, 0).start()
            if e % GROUP == 0:
                q_msg(e, 1).start()
    def kv_plane(n):
        return plane(jnp.where(lax.rem(n, 2) == 1, lax.div(n + 1, 2), -lax.div(n, 2)))

    def kv_out(n, kind):
        odd = lax.rem(n, 2) == 1
        slot = jnp.where(n == nz - 1, n, jnp.where(odd, n + 1, n - 1))
        zt = kv_plane(n)
        return pltpu.make_async_remote_copy(
            src_ref=kvp.at[target_heads(zt)[kind]], dst_ref=kvb.at[0, slot, x],
            send_sem=z_send.at[slot, kind], recv_sem=z_recv.at[slot],
            device_id={"blk": zt, "pair": kind}, device_id_type=MESH,
        )

    def send_kv(n):
        @pl.when(lax.div(kv_plane(n), half) == p)
        def _():
            kv_out(n, 0).start()
            kv_out(n, 1).start()

    window = 10

    @pl.loop(1, window + 1)
    def _(n):
        send_kv(n)

    ahead_hops = nx // 2
    behind_hops = nx - 1 - ahead_hops
    step = jnp.where(p == 0, 1, nx - 1)

    def column(n):
        return lax.rem(x + (n + nx) * (nx - step), nx)

    def hop(i, n):
        held = column(n - 1) if n > 0 else column(n + 1)
        return pltpu.make_async_remote_copy(
            src_ref=kvb.at[0, i, held], dst_ref=kvb.at[0, i, held],
            send_sem=x_send.at[i, n + behind_hops], recv_sem=x_recv.at[i, n + behind_hops],
            device_id={"node": column(-1 if n > 0 else 1)}, device_id_type=MESH,
        )

    def hop_arrived(i, n):
        got = column(n)
        pltpu.make_async_remote_copy(
            src_ref=kvb.at[0, i, got], dst_ref=kvb.at[0, i, got],
            send_sem=x_send.at[i, n + behind_hops], recv_sem=x_recv.at[i, n + behind_hops],
            device_id={"node": column(-1)}, device_id_type=MESH,
        ).wait_recv()

    def across(i, n):
        col = column(n)
        return pltpu.make_async_remote_copy(
            src_ref=kvb.at[0, i, col], dst_ref=kvb.at[1, i, col],
            send_sem=d_send.at[i, n + behind_hops], recv_sem=d_recv.at[i, n + behind_hops],
            device_id={"pair": 1 - p}, device_id_type=MESH,
        )

    def across_arrived(i, n):
        pltpu.make_async_remote_copy(
            src_ref=kvb.at[1, i, 0], dst_ref=kvb.at[1, i, 0],
            send_sem=d_send.at[i, n + behind_hops], recv_sem=d_recv.at[i, n + behind_hops],
            device_id={"pair": 1 - p}, device_id_type=MESH,
        ).wait_recv()

    def hand_over(i, n):
        @pl.when(p == 0)
        def _():
            across(i, n).start()

    def arrive(i):
        @pl.when((i == 0) & (side == p))
        def _():
            own_kv_local().wait()

        @pl.when((i > 0) | (side != p))
        def _():
            pltpu.make_async_remote_copy(
                src_ref=kvb.at[0, i, x], dst_ref=kvb.at[0, i, x],
                send_sem=z_send.at[0, 0], recv_sem=z_recv.at[i],
                device_id={"pair": 1 - p}, device_id_type=MESH,
            ).wait_recv()

        hop(i, 1).start()
        if behind_hops:
            hop(i, -1).start()
        hand_over(i, 0)

    def spread(i, n):
        hop_arrived(i, n)
        if n < ahead_hops:
            hop(i, n + 1).start()
        hand_over(i, n)
        if n <= behind_hops:
            hop_arrived(i, -n)
            if n < behind_hops:
                hop(i, -n - 1).start()
            hand_over(i, -n)

    width = 256
    spans = [(lo, min(lo + width, split), 1) for lo in range(0, split, width)]
    spans += [(hi, min(lo, nq), 0) for hi, lo in (
        [(split, up(split + 1, width))] + [(lo, lo + width) for lo in range(up(split + 1, width), nq, width)]
    ) if hi < nq]

    def compute(i):
        @pl.when(p == 1)
        def _():
            for n in range(-behind_hops, ahead_hops + 1):
                across_arrived(i, n)

        first = kvb[p, i].reshape(nx * rows, LANES)
        second = kvb[0, i].reshape(nx * rows, LANES)
        keys = (second, first)
        values = (second.T[HD:], first.T[HD:])

        def scored(span):
            lo, hi, kind = span
            sc = lax.dot_general(
                keys[kind], qrows[lo:hi, :], (((1,), (1,)), ((), ())),
                preferred_element_type=jnp.float32,
            )
            old = ml[0:1, lo:hi]
            return sc, old, jnp.maximum(old, jnp.max(sc, axis=0, keepdims=True))

        def weigh(span, sc, old, new):
            lo, hi, kind = span
            expo = jnp.exp2((sc - new) * scale2)
            factor = jnp.exp2((old - new) * scale2)
            total = ml[1:2, lo:hi] * factor + jnp.sum(expo, axis=0, keepdims=True)
            weighted = jnp.dot(
                values[kind], expo.astype(jnp.bfloat16), preferred_element_type=jnp.float32
            )
            return new, total, factor, weighted

        ready = scored(spans[0])
        results = []
        for n, span in enumerate(spans):
            following = scored(spans[n + 1]) if n + 1 < len(spans) else None
            results.append(weigh(span, *ready))
            ready = following
        for (lo, hi, _), (new, total, factor, weighted) in zip(spans, results):
            ml[0:1, lo:hi] = new
            ml[1:2, lo:hi] = total
            acc[:, lo:hi] = acc[:, lo:hi] * factor + weighted

    gap = 2
    for n in range(ahead_hops * gap + 1):
        arrive(n)

    def base(a):
        return pl.multiple_of(a * rows + jnp.where((p == 1) & (a >= far), split - far * rows, 0), 16)

    @pl.loop(0, messages)
    def _(a):
        own = (side == p) & (a == jnp.where(p == 0, 0, far))

        @pl.when(own)
        def _():
            own_q_local().wait()

        @pl.when(jnp.logical_not(own))
        def _():
            pltpu.make_async_remote_copy(
                src_ref=qin.at[a], dst_ref=qin.at[a], send_sem=q_send.at[0, 0],
                recv_sem=q_recv.at[a], device_id={"pair": 1 - p}, device_id_type=MESH,
            ).wait_recv()

        block = qin[a].astype(jnp.float32)
        both = jnp.concatenate(
            [jnp.where(low_half, block, 0.0), jnp.where(low_half, swap_sides(block), 0.0)], axis=0
        )
        qrows[pl.ds(base(a), rows), :] = both.astype(jnp.bfloat16)

    for m in range(1, ahead_hops + 1):
        for n in range((ahead_hops - m) * gap + 1):
            spread(n, m)

    @pl.loop(0, nz)
    def _(i):
        @pl.when(i + ahead_hops * gap + 1 < nz)
        def _():
            arrive(i + ahead_hops * gap + 1)

        @pl.when(i + window + 1 < nz)
        def _():
            send_kv(i + window + 1)

        for m in range(1, ahead_hops + 1):
            @pl.when(i + (ahead_hops - m) * gap + 1 < nz)
            def _():
                spread(i + (ahead_hops - m) * gap + 1, m)

        compute(i)

    def back(a):
        d = jnp.where(p == 0, offsets[a], (offsets[near:] + shared)[a])
        h = jnp.where((p == 1) & (a >= far), head_shared, head_own)
        return d, h

    def o_local(a):
        return pltpu.make_async_copy(ob.at[a], oin.at[back(a)[1]], own_sem.at[2])

    def o_msg(a):
        d, h = back(a)
        return pltpu.make_async_remote_copy(
            src_ref=ob.at[a], dst_ref=oin.at[h], send_sem=o_send.at[a], recv_sem=o_recv.at[h],
            device_id={"blk": plane(d), "pair": side}, device_id_type=MESH,
        )

    blank = jnp.zeros((LANES - HD, nq), jnp.float32)
    turned[...] = jnp.concatenate([acc[...] * (1.0 / ml[1:2, :]), blank], axis=0).T
    for a in range(messages):
        block = turned[pl.ds(base(a), rows), :]
        ob[a] = (block[:half_rows] + swap_sides(block[half_rows:])).astype(jnp.bfloat16)
        here = (back(a)[0] == 0) & (side == p)

        @pl.when(here)
        def _():
            o_local(a).start()

        @pl.when(jnp.logical_not(here))
        def _():
            o_msg(a).start()

    loads[3].wait()
    for i in range(tiles):
        for h in (2 * i, 2 * i + 1):
            g, n = divmod(h, GROUP + 1)
            zt = p * half + g * GROUP + (n if n < GROUP else lax.rem(z, GROUP))
            here = (zt == z) & (p == (0 if n < GROUP else 1))

            @pl.when(here)
            def _():
                pltpu.make_async_copy(ob.at[0], oin.at[h], own_sem.at[2]).wait()

            @pl.when(jnp.logical_not(here))
            def _():
                pltpu.make_async_remote_copy(
                    src_ref=oin.at[h], dst_ref=oin.at[h], send_sem=o_send.at[0],
                    recv_sem=o_recv.at[h], device_id={"pair": 1 - p}, device_id_type=MESH,
                ).wait_recv()

        even = oin[2 * i].astype(jnp.float32)
        odd = oin[2 * i + 1].astype(jnp.float32)
        cols = slice(i * LANES, (i + 1) * LANES)
        attn[0, :, cols] = jnp.where(low_half, even, swap_sides(odd)).astype(jnp.bfloat16)
        attn[1, :, cols] = jnp.where(low_half, swap_sides(even), odd).astype(jnp.bfloat16)

    sbuf[...] = jnp.dot(attn[1 - p], w[...], preferred_element_type=jnp.float32).astype(jnp.bfloat16)
    swap = pltpu.make_async_remote_copy(
        src_ref=sbuf, dst_ref=rbuf, send_sem=p_send, recv_sem=p_recv,
        device_id={"pair": 1 - p}, device_id_type=MESH,
    )
    swap.start()
    kept = jnp.dot(attn[p], w[...], preferred_element_type=jnp.float32)
    swap.wait_recv()
    out_ref[...] = (kept + rbuf[...].astype(jnp.float32)).astype(out_ref.dtype)
    swap.wait_send()

    @pl.when(side == p)
    def _():
        own_q_msg().wait_send()
        own_kv_msg().wait_send()

    for e in offsets[1:]:
        @pl.when(mine(e))
        def _():
            q_msg(e, 0).wait_send()
            if e % GROUP == 0:
                q_msg(e, 1).wait_send()
            kv_msg(e, 0).wait_send()
            kv_msg(e, 1).wait_send()

    @pl.loop(0, nz)
    def _(i):
        for n in range(1, ahead_hops + 1):
            hop(i, n).wait_send()
        for n in range(1, behind_hops + 1):
            hop(i, -n).wait_send()

        @pl.when(p == 0)
        def _():
            for n in range(-behind_hops, ahead_hops + 1):
                across(i, n).wait_send()

    for a in range(messages):
        @pl.when(jnp.logical_not((back(a)[0] == 0) & (side == p)))
        def _():
            o_msg(a).wait_send()


def solution(mesh):
    nz, nx = mesh.shape["blk"], mesh.shape["node"]

    def per_device(query, key, value, out_weight):
        rows, features = query.shape
        heads = features // HD
        assert nz % (2 * GROUP) == 0 and heads == nz // 2 // GROUP * (GROUP + 1)
        near = heads
        far = nz - near
        split = up(far * rows, LANES)
        nq = max(up(near * rows, LANES), split + up((nz // GROUP) * rows, LANES))
        out_features = out_weight.shape[1]
        dma = pltpu.SemaphoreType.DMA
        any_space = pl.BlockSpec(memory_space=pltpu.HBM)
        bf16, f32 = jnp.bfloat16, jnp.float32
        return pl.pallas_call(
            functools.partial(kernel, nz, nx, near),
            out_shape=jax.ShapeDtypeStruct((rows // 2, out_features), bf16),
            in_specs=[any_space] * 4,
            out_specs=pl.BlockSpec(memory_space=pltpu.VMEM),
            scratch_shapes=[
                pltpu.VMEM((rows, features), bf16),
                pltpu.VMEM((rows, features), bf16),
                pltpu.VMEM((rows, features), bf16),
                pltpu.VMEM((features, out_features), bf16),
                pltpu.VMEM((heads, rows, LANES), bf16),
                pltpu.VMEM((heads, rows // 2, LANES), bf16),
                pltpu.VMEM((2, nz, nx, rows, LANES), bf16),
                pltpu.VMEM((near, rows // 2, LANES), bf16),
                pltpu.VMEM((nq, LANES), bf16),
                pltpu.VMEM((2, nq), f32),
                pltpu.VMEM((HD, nq), f32),
                pltpu.VMEM((nq, LANES), f32),
                pltpu.VMEM((near, rows // 2, LANES), bf16),
                pltpu.VMEM((heads, rows // 2, LANES), bf16),
                pltpu.VMEM((2, rows // 2, features), bf16),
                pltpu.VMEM((rows // 2, out_features), bf16),
                pltpu.VMEM((rows // 2, out_features), bf16),
                dma((nz, 2)), dma((nz,)), dma((nz, 2)), dma((near,)),
                dma((nz, nx)), dma((nz, nx)), dma((nz, nx)), dma((nz, nx)),
                dma((near,)), dma((heads,)), dma, dma, dma((4,)), dma((3,)),
            ],
            compiler_params=pltpu.CompilerParams(
                collective_id=0, has_side_effects=True, vmem_limit_bytes=67043328 - 256 * 1024
            ),
        )(query, key, value, out_weight)

    tokens = P(("grp", "blk", "node"), "pair")
    return jax.shard_map(
        per_device,
        mesh=mesh,
        in_specs=(tokens, tokens, tokens, P("pair", None)),
        out_specs=P(("grp", "blk", "node", "pair"), None),
        check_vma=False,
    )
```

```python
import functools
import math

import jax
import jax.numpy as jnp
from jax import lax
from jax.experimental import pallas as pl
from jax.experimental.pallas import tpu as pltpu
from jax.sharding import PartitionSpec as P

HD = 64
LANES = 128
GROUP = 4
MESH = pl.DeviceIdType.MESH


def up(n, m):
    return -(-n // m) * m


def kernel(
    nz, nx, near, q_hbm, k_hbm, v_hbm, w_hbm, out_ref,
    q_in, k_in, v_in, w, kvp, qp, kvb, qin, qrows, ml, acc, turned, ob, oin, attn, sbuf, rbuf,
    z_send, z_recv, q_send, q_recv, x_send, x_recv, d_send, d_recv, o_send, o_recv,
    p_send, p_recv, loc, own_sem,
):
    rows, features = q_hbm.shape
    heads = features // HD
    tiles = features // LANES
    half_rows = rows // 2
    half = nz // 2
    z = lax.axis_index("blk")
    x = lax.axis_index("node")
    p = lax.axis_index("pair")
    scale2 = (1.0 / math.sqrt(HD)) * math.log2(math.e)
    offsets = [0]
    for d in range(1, half):
        offsets += [d, -d]
    offsets.append(half)
    shared = [d for d in offsets if d % GROUP == 0]
    far = nz - near
    messages = near
    side = lax.div(z, half)
    in_side = z - side * half
    lead = lax.div(in_side, GROUP) * (GROUP + 1)
    head_own = lead + lax.rem(in_side, GROUP)
    head_shared = lead + GROUP
    split = up(far * rows, LANES)
    nq = ml.shape[1]

    def plane(d):
        return lax.rem(z + nz + d, nz)

    def node(j):
        return lax.rem(x + j, nx)

    barrier = pltpu.get_barrier_semaphore()
    for d in offsets[1:]:
        for c in range(2):
            pl.semaphore_signal(
                barrier, inc=1, device_id={"blk": plane(d), "pair": c}, device_id_type=MESH
            )
    for j in range(1, nx):
        pl.semaphore_signal(barrier, inc=1, device_id={"node": node(j)}, device_id_type=MESH)
    pl.semaphore_signal(barrier, inc=1, device_id={"pair": 1 - p}, device_id_type=MESH)

    loads = [
        pltpu.make_async_copy(src, dst, loc.at[i])
        for i, (src, dst) in enumerate(((q_hbm, q_in), (k_hbm, k_in), (v_hbm, v_in), (w_hbm, w)))
    ]
    for load in loads:
        load.start()

    low = lax.broadcasted_iota(jnp.int32, (rows, LANES), 1) < HD
    low_half = lax.broadcasted_iota(jnp.int32, (half_rows, LANES), 1) < HD

    def swap_sides(a):
        return pltpu.roll(a, HD, 1)

    loads[0].wait()
    for i in range(tiles):
        tile = q_in[:, i * LANES:(i + 1) * LANES].astype(jnp.float32)
        top, bottom = tile[:half_rows], tile[half_rows:]
        qp[2 * i] = jnp.where(low_half, top, swap_sides(bottom)).astype(jnp.bfloat16)
        qp[2 * i + 1] = jnp.where(low_half, swap_sides(top), bottom).astype(jnp.bfloat16)
    loads[1].wait()
    loads[2].wait()
    for i in range(tiles):
        k_tile = k_in[:, i * LANES:(i + 1) * LANES].astype(jnp.float32)
        v_tile = v_in[:, i * LANES:(i + 1) * LANES].astype(jnp.float32)
        kvp[2 * i] = jnp.where(low, k_tile, swap_sides(v_tile)).astype(jnp.bfloat16)
        kvp[2 * i + 1] = jnp.where(low, swap_sides(k_tile), v_tile).astype(jnp.bfloat16)
    ml[0:1, :] = jnp.full((1, nq), -1e30, jnp.float32)
    ml[1:2, :] = jnp.zeros((1, nq), jnp.float32)
    acc[...] = jnp.zeros(acc.shape, jnp.float32)
    qrows[...] = jnp.zeros(qrows.shape, jnp.bfloat16)

    def full_place(d):
        i = offsets.index(d)
        return (0, i) if i < near else (1, i - near)

    def shared_place(d):
        return 1, far + shared.index(d)

    def opposite(e):
        return half if e == half else -e

    def target_heads(zt):
        first = lax.div(zt - p * half, GROUP) * (GROUP + 1)
        return first + lax.rem(zt, GROUP), first + GROUP

    def kv_msg(e, kind):
        slot = offsets.index(opposite(e))
        zt = plane(e)
        return pltpu.make_async_remote_copy(
            src_ref=kvp.at[target_heads(zt)[kind]], dst_ref=kvb.at[0, slot, x],
            send_sem=z_send.at[slot, kind], recv_sem=z_recv.at[slot],
            device_id={"blk": zt, "pair": kind}, device_id_type=MESH,
        )

    def q_msg(e, kind):
        zt = plane(e)
        core, place = (full_place, shared_place)[kind](opposite(e))
        return pltpu.make_async_remote_copy(
            src_ref=qp.at[target_heads(zt)[kind]], dst_ref=qin.at[place],
            send_sem=q_send.at[offsets.index(e), kind], recv_sem=q_recv.at[place],
            device_id={"blk": zt, "pair": core}, device_id_type=MESH,
        )

    def mine(e):
        return lax.div(plane(e), half) == p

    def own_kv_local():
        return pltpu.make_async_copy(
            kvp.at[jnp.where(p == 0, head_own, head_shared)], kvb.at[0, 0, x], own_sem.at[0]
        )

    def own_kv_msg():
        return pltpu.make_async_remote_copy(
            src_ref=kvp.at[jnp.where(p == 0, head_shared, head_own)], dst_ref=kvb.at[0, 0, x],
            send_sem=z_send.at[0, 0], recv_sem=z_recv.at[0],
            device_id={"pair": 1 - p}, device_id_type=MESH,
        )

    def own_q_local():
        return pltpu.make_async_copy(
            qp.at[jnp.where(p == 0, head_own, head_shared)],
            qin.at[jnp.where(p == 0, 0, far)], own_sem.at[1],
        )

    def own_q_msg():
        there = jnp.where(p == 0, far, 0)
        return pltpu.make_async_remote_copy(
            src_ref=qp.at[jnp.where(p == 0, head_shared, head_own)], dst_ref=qin.at[there],
            send_sem=q_send.at[0, 0], recv_sem=q_recv.at[there],
            device_id={"pair": 1 - p}, device_id_type=MESH,
        )

    pl.semaphore_wait(barrier, 2 * (nz - 1) + nx)

    @pl.when(side == p)
    def _():
        own_q_local().start()
        own_kv_local().start()
        own_q_msg().start()
        own_kv_msg().start()

    for e in offsets[1:]:
        @pl.when(mine(e))
        def _():
            q_msg(e, 0).start()
            if e % GROUP == 0:
                q_msg(e, 1).start()
    def kv_plane(n):
        return plane(jnp.where(lax.rem(n, 2) == 1, lax.div(n + 1, 2), -lax.div(n, 2)))

    def kv_out(n, kind):
        odd = lax.rem(n, 2) == 1
        slot = jnp.where(n == nz - 1, n, jnp.where(odd, n + 1, n - 1))
        zt = kv_plane(n)
        return pltpu.make_async_remote_copy(
            src_ref=kvp.at[target_heads(zt)[kind]], dst_ref=kvb.at[0, slot, x],
            send_sem=z_send.at[slot, kind], recv_sem=z_recv.at[slot],
            device_id={"blk": zt, "pair": kind}, device_id_type=MESH,
        )

    def send_kv(n):
        @pl.when(lax.div(kv_plane(n), half) == p)
        def _():
            kv_out(n, 0).start()
            kv_out(n, 1).start()

    window = 10

    @pl.loop(1, window + 1)
    def _(n):
        send_kv(n)

    ahead_hops = nx // 2
    behind_hops = nx - 1 - ahead_hops
    step = jnp.where(p == 0, 1, nx - 1)

    def column(n):
        return lax.rem(x + (n + nx) * (nx - step), nx)

    def hop(i, n):
        held = column(n - 1) if n > 0 else column(n + 1)
        return pltpu.make_async_remote_copy(
            src_ref=kvb.at[0, i, held], dst_ref=kvb.at[0, i, held],
            send_sem=x_send.at[i, n + behind_hops], recv_sem=x_recv.at[i, n + behind_hops],
            device_id={"node": column(-1 if n > 0 else 1)}, device_id_type=MESH,
        )

    def hop_arrived(i, n):
        got = column(n)
        pltpu.make_async_remote_copy(
            src_ref=kvb.at[0, i, got], dst_ref=kvb.at[0, i, got],
            send_sem=x_send.at[i, n + behind_hops], recv_sem=x_recv.at[i, n + behind_hops],
            device_id={"node": column(-1)}, device_id_type=MESH,
        ).wait_recv()

    def across(i, n):
        col = column(n)
        return pltpu.make_async_remote_copy(
            src_ref=kvb.at[0, i, col], dst_ref=kvb.at[1, i, col],
            send_sem=d_send.at[i, n + behind_hops], recv_sem=d_recv.at[i, n + behind_hops],
            device_id={"pair": 1 - p}, device_id_type=MESH,
        )

    def across_arrived(i, n):
        pltpu.make_async_remote_copy(
            src_ref=kvb.at[1, i, 0], dst_ref=kvb.at[1, i, 0],
            send_sem=d_send.at[i, n + behind_hops], recv_sem=d_recv.at[i, n + behind_hops],
            device_id={"pair": 1 - p}, device_id_type=MESH,
        ).wait_recv()

    def hand_over(i, n):
        @pl.when(p == 0)
        def _():
            across(i, n).start()

    def arrive(i):
        @pl.when((i == 0) & (side == p))
        def _():
            own_kv_local().wait()

        @pl.when((i > 0) | (side != p))
        def _():
            pltpu.make_async_remote_copy(
                src_ref=kvb.at[0, i, x], dst_ref=kvb.at[0, i, x],
                send_sem=z_send.at[0, 0], recv_sem=z_recv.at[i],
                device_id={"pair": 1 - p}, device_id_type=MESH,
            ).wait_recv()

        hop(i, 1).start()
        if behind_hops:
            hop(i, -1).start()
        hand_over(i, 0)

    def spread(i, n):
        hop_arrived(i, n)
        if n < ahead_hops:
            hop(i, n + 1).start()
        hand_over(i, n)
        if n <= behind_hops:
            hop_arrived(i, -n)
            if n < behind_hops:
                hop(i, -n - 1).start()
            hand_over(i, -n)

    width = 256
    spans = [(lo, min(lo + width, split), 1) for lo in range(0, split, width)]
    spans += [(hi, min(lo, nq), 0) for hi, lo in (
        [(split, up(split + 1, width))] + [(lo, lo + width) for lo in range(up(split + 1, width), nq, width)]
    ) if hi < nq]

    def compute(i):
        @pl.when(p == 1)
        def _():
            for n in range(-behind_hops, ahead_hops + 1):
                across_arrived(i, n)

        first = kvb[p, i].reshape(nx * rows, LANES)
        second = kvb[0, i].reshape(nx * rows, LANES)
        keys = (second, first)
        values = (second.T[HD:], first.T[HD:])

        def scored(span):
            lo, hi, kind = span
            sc = lax.dot_general(
                keys[kind], qrows[lo:hi, :], (((1,), (1,)), ((), ())),
                preferred_element_type=jnp.float32,
            )
            old = ml[0:1, lo:hi]
            return sc, old, jnp.maximum(old, jnp.max(sc, axis=0, keepdims=True))

        def weigh(span, sc, old, new):
            lo, hi, kind = span
            expo = jnp.exp2((sc - new) * scale2)
            factor = jnp.exp2((old - new) * scale2)
            total = ml[1:2, lo:hi] * factor + jnp.sum(expo, axis=0, keepdims=True)
            weighted = jnp.dot(
                values[kind], expo.astype(jnp.bfloat16), preferred_element_type=jnp.float32
            )
            return new, total, factor, weighted

        ready = scored(spans[0])
        results = []
        for n, span in enumerate(spans):
            following = scored(spans[n + 1]) if n + 1 < len(spans) else None
            results.append(weigh(span, *ready))
            ready = following
        for (lo, hi, _), (new, total, factor, weighted) in zip(spans, results):
            ml[0:1, lo:hi] = new
            ml[1:2, lo:hi] = total
            acc[:, lo:hi] = acc[:, lo:hi] * factor + weighted

    gap = 2
    for n in range(ahead_hops * gap + 1):
        arrive(n)

    def base(a):
        return pl.multiple_of(a * rows + jnp.where((p == 1) & (a >= far), split - far * rows, 0), 16)

    @pl.loop(0, messages)
    def _(a):
        own = (side == p) & (a == jnp.where(p == 0, 0, far))

        @pl.when(own)
        def _():
            own_q_local().wait()

        @pl.when(jnp.logical_not(own))
        def _():
            pltpu.make_async_remote_copy(
                src_ref=qin.at[a], dst_ref=qin.at[a], send_sem=q_send.at[0, 0],
                recv_sem=q_recv.at[a], device_id={"pair": 1 - p}, device_id_type=MESH,
            ).wait_recv()

        block = qin[a].astype(jnp.float32)
        both = jnp.concatenate(
            [jnp.where(low_half, block, 0.0), jnp.where(low_half, swap_sides(block), 0.0)], axis=0
        )
        qrows[pl.ds(base(a), rows), :] = both.astype(jnp.bfloat16)

    for m in range(1, ahead_hops + 1):
        for n in range((ahead_hops - m) * gap + 1):
            spread(n, m)

    lead_in = ahead_hops * gap + 1
    tail = nz - lead_in + 2

    def stage_end(n, m):
        slack = (m - 1) * (gap - 1) + 1 if m <= ahead_hops else ahead_hops * (gap - 1)
        late = jnp.clip(n - tail + 1, 0, slack)
        return jnp.clip(n + 1 - gap * min(m, ahead_hops) - (m > ahead_hops) + late, 0, nz)

    @pl.loop(lead_in, nz + ahead_hops + 1)
    def _(n):
        @pl.when(n < nz)
        def _():
            arrive(n)

        @pl.when(n - lead_in + window + 1 < nz)
        def _():
            send_kv(n - lead_in + window + 1)

        for m in range(1, ahead_hops + 1):
            @pl.loop(stage_end(n - 1, m), stage_end(n, m))
            def _(k):
                spread(k, m)

        @pl.loop(stage_end(n - 1, ahead_hops + 1), stage_end(n, ahead_hops + 1))
        def _(k):
            compute(k)

    def back(a):
        d = jnp.where(p == 0, offsets[a], (offsets[near:] + shared)[a])
        h = jnp.where((p == 1) & (a >= far), head_shared, head_own)
        return d, h

    def o_local(a):
        return pltpu.make_async_copy(ob.at[a], oin.at[back(a)[1]], own_sem.at[2])

    def o_msg(a):
        d, h = back(a)
        return pltpu.make_async_remote_copy(
            src_ref=ob.at[a], dst_ref=oin.at[h], send_sem=o_send.at[a], recv_sem=o_recv.at[h],
            device_id={"blk": plane(d), "pair": side}, device_id_type=MESH,
        )

    blank = jnp.zeros((LANES - HD, nq), jnp.float32)
    turned[...] = jnp.concatenate([acc[...] * (1.0 / ml[1:2, :]), blank], axis=0).T
    for a in range(messages):
        block = turned[pl.ds(base(a), rows), :]
        ob[a] = (block[:half_rows] + swap_sides(block[half_rows:])).astype(jnp.bfloat16)
        here = (back(a)[0] == 0) & (side == p)

        @pl.when(here)
        def _():
            o_local(a).start()

        @pl.when(jnp.logical_not(here))
        def _():
            o_msg(a).start()

    loads[3].wait()
    for i in range(tiles):
        for h in (2 * i, 2 * i + 1):
            g, n = divmod(h, GROUP + 1)
            zt = p * half + g * GROUP + (n if n < GROUP else lax.rem(z, GROUP))
            here = (zt == z) & (p == (0 if n < GROUP else 1))

            @pl.when(here)
            def _():
                pltpu.make_async_copy(ob.at[0], oin.at[h], own_sem.at[2]).wait()

            @pl.when(jnp.logical_not(here))
            def _():
                pltpu.make_async_remote_copy(
                    src_ref=oin.at[h], dst_ref=oin.at[h], send_sem=o_send.at[0],
                    recv_sem=o_recv.at[h], device_id={"pair": 1 - p}, device_id_type=MESH,
                ).wait_recv()

        even = oin[2 * i].astype(jnp.float32)
        odd = oin[2 * i + 1].astype(jnp.float32)
        cols = slice(i * LANES, (i + 1) * LANES)
        attn[0, :, cols] = jnp.where(low_half, even, swap_sides(odd)).astype(jnp.bfloat16)
        attn[1, :, cols] = jnp.where(low_half, swap_sides(even), odd).astype(jnp.bfloat16)

    sbuf[...] = jnp.dot(attn[1 - p], w[...], preferred_element_type=jnp.float32).astype(jnp.bfloat16)
    swap = pltpu.make_async_remote_copy(
        src_ref=sbuf, dst_ref=rbuf, send_sem=p_send, recv_sem=p_recv,
        device_id={"pair": 1 - p}, device_id_type=MESH,
    )
    swap.start()
    kept = jnp.dot(attn[p], w[...], preferred_element_type=jnp.float32)
    swap.wait_recv()
    out_ref[...] = (kept + rbuf[...].astype(jnp.float32)).astype(out_ref.dtype)
    swap.wait_send()

    @pl.when(side == p)
    def _():
        own_q_msg().wait_send()
        own_kv_msg().wait_send()

    for e in offsets[1:]:
        @pl.when(mine(e))
        def _():
            q_msg(e, 0).wait_send()
            if e % GROUP == 0:
                q_msg(e, 1).wait_send()
            kv_msg(e, 0).wait_send()
            kv_msg(e, 1).wait_send()

    @pl.loop(0, nz)
    def _(i):
        for n in range(1, ahead_hops + 1):
            hop(i, n).wait_send()
        for n in range(1, behind_hops + 1):
            hop(i, -n).wait_send()

        @pl.when(p == 0)
        def _():
            for n in range(-behind_hops, ahead_hops + 1):
                across(i, n).wait_send()

    for a in range(messages):
        @pl.when(jnp.logical_not((back(a)[0] == 0) & (side == p)))
        def _():
            o_msg(a).wait_send()


def solution(mesh):
    nz, nx = mesh.shape["blk"], mesh.shape["node"]

    def per_device(query, key, value, out_weight):
        rows, features = query.shape
        heads = features // HD
        assert nz % (2 * GROUP) == 0 and heads == nz // 2 // GROUP * (GROUP + 1)
        near = heads
        far = nz - near
        split = up(far * rows, LANES)
        nq = max(up(near * rows, LANES), split + up((nz // GROUP) * rows, LANES))
        out_features = out_weight.shape[1]
        dma = pltpu.SemaphoreType.DMA
        any_space = pl.BlockSpec(memory_space=pltpu.HBM)
        bf16, f32 = jnp.bfloat16, jnp.float32
        return pl.pallas_call(
            functools.partial(kernel, nz, nx, near),
            out_shape=jax.ShapeDtypeStruct((rows // 2, out_features), bf16),
            in_specs=[any_space] * 4,
            out_specs=pl.BlockSpec(memory_space=pltpu.VMEM),
            scratch_shapes=[
                pltpu.VMEM((rows, features), bf16),
                pltpu.VMEM((rows, features), bf16),
                pltpu.VMEM((rows, features), bf16),
                pltpu.VMEM((features, out_features), bf16),
                pltpu.VMEM((heads, rows, LANES), bf16),
                pltpu.VMEM((heads, rows // 2, LANES), bf16),
                pltpu.VMEM((2, nz, nx, rows, LANES), bf16),
                pltpu.VMEM((near, rows // 2, LANES), bf16),
                pltpu.VMEM((nq, LANES), bf16),
                pltpu.VMEM((2, nq), f32),
                pltpu.VMEM((HD, nq), f32),
                pltpu.VMEM((nq, LANES), f32),
                pltpu.VMEM((near, rows // 2, LANES), bf16),
                pltpu.VMEM((heads, rows // 2, LANES), bf16),
                pltpu.VMEM((2, rows // 2, features), bf16),
                pltpu.VMEM((rows // 2, out_features), bf16),
                pltpu.VMEM((rows // 2, out_features), bf16),
                dma((nz, 2)), dma((nz,)), dma((nz, 2)), dma((near,)),
                dma((nz, nx)), dma((nz, nx)), dma((nz, nx)), dma((nz, nx)),
                dma((near,)), dma((heads,)), dma, dma, dma((4,)), dma((3,)),
            ],
            compiler_params=pltpu.CompilerParams(
                collective_id=0, has_side_effects=True, vmem_limit_bytes=67043328 - 256 * 1024
            ),
        )(query, key, value, out_weight)

    tokens = P(("grp", "blk", "node"), "pair")
    return jax.shard_map(
        per_device,
        mesh=mesh,
        in_specs=(tokens, tokens, tokens, P("pair", None)),
        out_specs=P(("grp", "blk", "node", "pair"), None),
        check_vma=False,
    )
```

```python
import functools
import math

import jax
import jax.numpy as jnp
from jax import lax
from jax.experimental import pallas as pl
from jax.experimental.pallas import tpu as pltpu
from jax.sharding import PartitionSpec as P

HD = 64
LANES = 128
GROUP = 4
MESH = pl.DeviceIdType.MESH


def up(n, m):
    return -(-n // m) * m


def kernel(
    nz, nx, near, q_hbm, k_hbm, v_hbm, w_hbm, out_ref,
    q_in, k_in, v_in, w, kvp, qp, kvb, qin, qrows, ml, acc, turned, ob, oin, attn, sbuf, rbuf,
    z_send, z_recv, q_send, q_recv, x_send, x_recv, d_send, d_recv, o_send, o_recv,
    p_send, p_recv, loc, own_sem,
):
    rows, features = q_hbm.shape
    heads = features // HD
    tiles = features // LANES
    half_rows = rows // 2
    half = nz // 2
    z = lax.axis_index("blk")
    x = lax.axis_index("node")
    p = lax.axis_index("pair")
    scale2 = (1.0 / math.sqrt(HD)) * math.log2(math.e)
    offsets = [0]
    for d in range(1, half):
        offsets += [d, -d]
    offsets.append(half)
    shared = [d for d in offsets if d % GROUP == 0]
    far = nz - near
    messages = near
    side = lax.div(z, half)
    in_side = z - side * half
    lead = lax.div(in_side, GROUP) * (GROUP + 1)
    head_own = lead + lax.rem(in_side, GROUP)
    head_shared = lead + GROUP
    split = up(far * rows, LANES)
    nq = ml.shape[1]

    def plane(d):
        return lax.rem(z + nz + d, nz)

    def node(j):
        return lax.rem(x + j, nx)

    barrier = pltpu.get_barrier_semaphore()
    for d in offsets[1:]:
        for c in range(2):
            pl.semaphore_signal(
                barrier, inc=1, device_id={"blk": plane(d), "pair": c}, device_id_type=MESH
            )
    for j in range(1, nx):
        pl.semaphore_signal(barrier, inc=1, device_id={"node": node(j)}, device_id_type=MESH)
    pl.semaphore_signal(barrier, inc=1, device_id={"pair": 1 - p}, device_id_type=MESH)

    loads = [
        pltpu.make_async_copy(src, dst, loc.at[i])
        for i, (src, dst) in enumerate(((q_hbm, q_in), (k_hbm, k_in), (v_hbm, v_in), (w_hbm, w)))
    ]
    for load in loads:
        load.start()

    low = lax.broadcasted_iota(jnp.int32, (rows, LANES), 1) < HD
    low_half = lax.broadcasted_iota(jnp.int32, (half_rows, LANES), 1) < HD

    def swap_sides(a):
        return pltpu.roll(a, HD, 1)

    loads[0].wait()
    for i in range(tiles):
        tile = q_in[:, i * LANES:(i + 1) * LANES].astype(jnp.float32)
        top, bottom = tile[:half_rows], tile[half_rows:]
        qp[2 * i] = jnp.where(low_half, top, swap_sides(bottom)).astype(jnp.bfloat16)
        qp[2 * i + 1] = jnp.where(low_half, swap_sides(top), bottom).astype(jnp.bfloat16)
    loads[1].wait()
    loads[2].wait()
    for i in range(tiles):
        k_tile = k_in[:, i * LANES:(i + 1) * LANES].astype(jnp.float32)
        v_tile = v_in[:, i * LANES:(i + 1) * LANES].astype(jnp.float32)
        kvp[2 * i] = jnp.where(low, k_tile, swap_sides(v_tile)).astype(jnp.bfloat16)
        kvp[2 * i + 1] = jnp.where(low, swap_sides(k_tile), v_tile).astype(jnp.bfloat16)
    ml[0:1, :] = jnp.full((1, nq), -1e30, jnp.float32)
    ml[1:2, :] = jnp.zeros((1, nq), jnp.float32)
    acc[...] = jnp.zeros(acc.shape, jnp.float32)
    qrows[...] = jnp.zeros(qrows.shape, jnp.bfloat16)

    def full_place(d):
        i = offsets.index(d)
        return (0, i) if i < near else (1, i - near)

    def shared_place(d):
        return 1, far + shared.index(d)

    def opposite(e):
        return half if e == half else -e

    def target_heads(zt):
        first = lax.div(zt - p * half, GROUP) * (GROUP + 1)
        return first + lax.rem(zt, GROUP), first + GROUP

    def kv_msg(e, kind):
        slot = offsets.index(opposite(e))
        zt = plane(e)
        return pltpu.make_async_remote_copy(
            src_ref=kvp.at[target_heads(zt)[kind]], dst_ref=kvb.at[0, slot, x],
            send_sem=z_send.at[slot, kind], recv_sem=z_recv.at[slot],
            device_id={"blk": zt, "pair": kind}, device_id_type=MESH,
        )

    def q_msg(e, kind):
        zt = plane(e)
        core, place = (full_place, shared_place)[kind](opposite(e))
        return pltpu.make_async_remote_copy(
            src_ref=qp.at[target_heads(zt)[kind]], dst_ref=qin.at[place],
            send_sem=q_send.at[offsets.index(e), kind], recv_sem=q_recv.at[place],
            device_id={"blk": zt, "pair": core}, device_id_type=MESH,
        )

    def mine(e):
        return lax.div(plane(e), half) == p

    def own_kv_local():
        return pltpu.make_async_copy(
            kvp.at[jnp.where(p == 0, head_own, head_shared)], kvb.at[0, 0, x], own_sem.at[0]
        )

    def own_kv_msg():
        return pltpu.make_async_remote_copy(
            src_ref=kvp.at[jnp.where(p == 0, head_shared, head_own)], dst_ref=kvb.at[0, 0, x],
            send_sem=z_send.at[0, 0], recv_sem=z_recv.at[0],
            device_id={"pair": 1 - p}, device_id_type=MESH,
        )

    def own_q_local():
        return pltpu.make_async_copy(
            qp.at[jnp.where(p == 0, head_own, head_shared)],
            qin.at[jnp.where(p == 0, 0, far)], own_sem.at[1],
        )

    def own_q_msg():
        there = jnp.where(p == 0, far, 0)
        return pltpu.make_async_remote_copy(
            src_ref=qp.at[jnp.where(p == 0, head_shared, head_own)], dst_ref=qin.at[there],
            send_sem=q_send.at[0, 0], recv_sem=q_recv.at[there],
            device_id={"pair": 1 - p}, device_id_type=MESH,
        )

    pl.semaphore_wait(barrier, 2 * (nz - 1) + nx)

    @pl.when(side == p)
    def _():
        own_q_local().start()
        own_kv_local().start()
        own_q_msg().start()
        own_kv_msg().start()

    for e in offsets[1:]:
        @pl.when(mine(e))
        def _():
            q_msg(e, 0).start()
            if e % GROUP == 0:
                q_msg(e, 1).start()
    def kv_plane(n):
        return plane(jnp.where(lax.rem(n, 2) == 1, lax.div(n + 1, 2), -lax.div(n, 2)))

    def kv_out(n, kind):
        odd = lax.rem(n, 2) == 1
        slot = jnp.where(n == nz - 1, n, jnp.where(odd, n + 1, n - 1))
        zt = kv_plane(n)
        return pltpu.make_async_remote_copy(
            src_ref=kvp.at[target_heads(zt)[kind]], dst_ref=kvb.at[0, slot, x],
            send_sem=z_send.at[slot, kind], recv_sem=z_recv.at[slot],
            device_id={"blk": zt, "pair": kind}, device_id_type=MESH,
        )

    def send_kv(n):
        @pl.when(lax.div(kv_plane(n), half) == p)
        def _():
            kv_out(n, 0).start()
            kv_out(n, 1).start()

    window = 12

    @pl.loop(1, window + 1)
    def _(n):
        send_kv(n)

    ahead_hops = nx // 2
    behind_hops = nx - 1 - ahead_hops
    step = jnp.where(p == 0, 1, nx - 1)

    def column(n):
        return lax.rem(x + (n + nx) * (nx - step), nx)

    def hop(i, n):
        held = column(n - 1) if n > 0 else column(n + 1)
        return pltpu.make_async_remote_copy(
            src_ref=kvb.at[0, i, held], dst_ref=kvb.at[0, i, held],
            send_sem=x_send.at[i, n + behind_hops], recv_sem=x_recv.at[i, n + behind_hops],
            device_id={"node": column(-1 if n > 0 else 1)}, device_id_type=MESH,
        )

    def hop_arrived(i, n):
        got = column(n)
        pltpu.make_async_remote_copy(
            src_ref=kvb.at[0, i, got], dst_ref=kvb.at[0, i, got],
            send_sem=x_send.at[i, n + behind_hops], recv_sem=x_recv.at[i, n + behind_hops],
            device_id={"node": column(-1)}, device_id_type=MESH,
        ).wait_recv()

    def across(i, n):
        col = column(n)
        return pltpu.make_async_remote_copy(
            src_ref=kvb.at[0, i, col], dst_ref=kvb.at[1, i, col],
            send_sem=d_send.at[i, n + behind_hops], recv_sem=d_recv.at[i, n + behind_hops],
            device_id={"pair": 1 - p}, device_id_type=MESH,
        )

    def across_arrived(i, n):
        pltpu.make_async_remote_copy(
            src_ref=kvb.at[1, i, 0], dst_ref=kvb.at[1, i, 0],
            send_sem=d_send.at[i, n + behind_hops], recv_sem=d_recv.at[i, n + behind_hops],
            device_id={"pair": 1 - p}, device_id_type=MESH,
        ).wait_recv()

    def hand_over(i, n):
        @pl.when(p == 0)
        def _():
            across(i, n).start()

    def arrive(i):
        @pl.when((i == 0) & (side == p))
        def _():
            own_kv_local().wait()

        @pl.when((i > 0) | (side != p))
        def _():
            pltpu.make_async_remote_copy(
                src_ref=kvb.at[0, i, x], dst_ref=kvb.at[0, i, x],
                send_sem=z_send.at[0, 0], recv_sem=z_recv.at[i],
                device_id={"pair": 1 - p}, device_id_type=MESH,
            ).wait_recv()

        hop(i, 1).start()
        if behind_hops:
            hop(i, -1).start()
        hand_over(i, 0)

    def spread(i, n):
        hop_arrived(i, n)
        if n < ahead_hops:
            hop(i, n + 1).start()
        hand_over(i, n)
        if n <= behind_hops:
            hop_arrived(i, -n)
            if n < behind_hops:
                hop(i, -n - 1).start()
            hand_over(i, -n)

    width = 256
    spans = [(lo, min(lo + width, split), 1) for lo in range(0, split, width)]
    spans += [(hi, min(lo, nq), 0) for hi, lo in (
        [(split, up(split + 1, width))] + [(lo, lo + width) for lo in range(up(split + 1, width), nq, width)]
    ) if hi < nq]

    def compute(i):
        @pl.when(p == 1)
        def _():
            for n in range(-behind_hops, ahead_hops + 1):
                across_arrived(i, n)

        first = kvb[p, i].reshape(nx * rows, LANES)
        second = kvb[0, i].reshape(nx * rows, LANES)
        keys = (second, first)
        values = (second.T[HD:], first.T[HD:])

        def scored(span):
            lo, hi, kind = span
            sc = lax.dot_general(
                keys[kind], qrows[lo:hi, :], (((1,), (1,)), ((), ())),
                preferred_element_type=jnp.float32,
            )
            old = ml[0:1, lo:hi]
            return sc, old, jnp.maximum(old, jnp.max(sc, axis=0, keepdims=True))

        def weigh(span, sc, old, new):
            lo, hi, kind = span
            expo = jnp.exp2((sc - new) * scale2)
            factor = jnp.exp2((old - new) * scale2)
            total = ml[1:2, lo:hi] * factor + jnp.sum(expo, axis=0, keepdims=True)
            weighted = jnp.dot(
                values[kind], expo.astype(jnp.bfloat16), preferred_element_type=jnp.float32
            )
            return new, total, factor, weighted

        ready = scored(spans[0])
        results = []
        for n, span in enumerate(spans):
            following = scored(spans[n + 1]) if n + 1 < len(spans) else None
            results.append(weigh(span, *ready))
            ready = following
        for (lo, hi, _), (new, total, factor, weighted) in zip(spans, results):
            ml[0:1, lo:hi] = new
            ml[1:2, lo:hi] = total
            acc[:, lo:hi] = acc[:, lo:hi] * factor + weighted

    gap = 3
    for n in range(ahead_hops * gap + 1):
        arrive(n)

    def base(a):
        return pl.multiple_of(a * rows + jnp.where((p == 1) & (a >= far), split - far * rows, 0), 16)

    @pl.loop(0, messages)
    def _(a):
        own = (side == p) & (a == jnp.where(p == 0, 0, far))

        @pl.when(own)
        def _():
            own_q_local().wait()

        @pl.when(jnp.logical_not(own))
        def _():
            pltpu.make_async_remote_copy(
                src_ref=qin.at[a], dst_ref=qin.at[a], send_sem=q_send.at[0, 0],
                recv_sem=q_recv.at[a], device_id={"pair": 1 - p}, device_id_type=MESH,
            ).wait_recv()

        block = qin[a].astype(jnp.float32)
        both = jnp.concatenate(
            [jnp.where(low_half, block, 0.0), jnp.where(low_half, swap_sides(block), 0.0)], axis=0
        )
        qrows[pl.ds(base(a), rows), :] = both.astype(jnp.bfloat16)

    for m in range(1, ahead_hops + 1):
        for n in range((ahead_hops - m) * gap + 1):
            spread(n, m)

    @pl.loop(0, nz)
    def _(i):
        @pl.when(i + ahead_hops * gap + 1 < nz)
        def _():
            arrive(i + ahead_hops * gap + 1)

        @pl.when(i + window + 1 < nz)
        def _():
            send_kv(i + window + 1)

        for m in range(1, ahead_hops + 1):
            @pl.when(i + (ahead_hops - m) * gap + 1 < nz)
            def _():
                spread(i + (ahead_hops - m) * gap + 1, m)

        compute(i)

    def back(a):
        d = jnp.where(p == 0, offsets[a], (offsets[near:] + shared)[a])
        h = jnp.where((p == 1) & (a >= far), head_shared, head_own)
        return d, h

    def o_local(a):
        return pltpu.make_async_copy(ob.at[a], oin.at[back(a)[1]], own_sem.at[2])

    def o_msg(a):
        d, h = back(a)
        return pltpu.make_async_remote_copy(
            src_ref=ob.at[a], dst_ref=oin.at[h], send_sem=o_send.at[a], recv_sem=o_recv.at[h],
            device_id={"blk": plane(d), "pair": side}, device_id_type=MESH,
        )

    blank = jnp.zeros((LANES - HD, nq), jnp.float32)
    turned[...] = jnp.concatenate([acc[...] * (1.0 / ml[1:2, :]), blank], axis=0).T
    for a in range(messages):
        block = turned[pl.ds(base(a), rows), :]
        ob[a] = (block[:half_rows] + swap_sides(block[half_rows:])).astype(jnp.bfloat16)
        here = (back(a)[0] == 0) & (side == p)

        @pl.when(here)
        def _():
            o_local(a).start()

        @pl.when(jnp.logical_not(here))
        def _():
            o_msg(a).start()

    loads[3].wait()
    for i in range(tiles):
        for h in (2 * i, 2 * i + 1):
            g, n = divmod(h, GROUP + 1)
            zt = p * half + g * GROUP + (n if n < GROUP else lax.rem(z, GROUP))
            here = (zt == z) & (p == (0 if n < GROUP else 1))

            @pl.when(here)
            def _():
                pltpu.make_async_copy(ob.at[0], oin.at[h], own_sem.at[2]).wait()

            @pl.when(jnp.logical_not(here))
            def _():
                pltpu.make_async_remote_copy(
                    src_ref=oin.at[h], dst_ref=oin.at[h], send_sem=o_send.at[0],
                    recv_sem=o_recv.at[h], device_id={"pair": 1 - p}, device_id_type=MESH,
                ).wait_recv()

        even = oin[2 * i].astype(jnp.float32)
        odd = oin[2 * i + 1].astype(jnp.float32)
        cols = slice(i * LANES, (i + 1) * LANES)
        attn[0, :, cols] = jnp.where(low_half, even, swap_sides(odd)).astype(jnp.bfloat16)
        attn[1, :, cols] = jnp.where(low_half, swap_sides(even), odd).astype(jnp.bfloat16)

    sbuf[...] = jnp.dot(attn[1 - p], w[...], preferred_element_type=jnp.float32).astype(jnp.bfloat16)
    swap = pltpu.make_async_remote_copy(
        src_ref=sbuf, dst_ref=rbuf, send_sem=p_send, recv_sem=p_recv,
        device_id={"pair": 1 - p}, device_id_type=MESH,
    )
    swap.start()
    kept = jnp.dot(attn[p], w[...], preferred_element_type=jnp.float32)
    swap.wait_recv()
    out_ref[...] = (kept + rbuf[...].astype(jnp.float32)).astype(out_ref.dtype)
    swap.wait_send()

    @pl.when(side == p)
    def _():
        own_q_msg().wait_send()
        own_kv_msg().wait_send()

    for e in offsets[1:]:
        @pl.when(mine(e))
        def _():
            q_msg(e, 0).wait_send()
            if e % GROUP == 0:
                q_msg(e, 1).wait_send()
            kv_msg(e, 0).wait_send()
            kv_msg(e, 1).wait_send()

    @pl.loop(0, nz)
    def _(i):
        for n in range(1, ahead_hops + 1):
            hop(i, n).wait_send()
        for n in range(1, behind_hops + 1):
            hop(i, -n).wait_send()

        @pl.when(p == 0)
        def _():
            for n in range(-behind_hops, ahead_hops + 1):
                across(i, n).wait_send()

    for a in range(messages):
        @pl.when(jnp.logical_not((back(a)[0] == 0) & (side == p)))
        def _():
            o_msg(a).wait_send()


def solution(mesh):
    nz, nx = mesh.shape["blk"], mesh.shape["node"]

    def per_device(query, key, value, out_weight):
        rows, features = query.shape
        heads = features // HD
        assert nz % (2 * GROUP) == 0 and heads == nz // 2 // GROUP * (GROUP + 1)
        near = heads
        far = nz - near
        split = up(far * rows, LANES)
        nq = max(up(near * rows, LANES), split + up((nz // GROUP) * rows, LANES))
        out_features = out_weight.shape[1]
        dma = pltpu.SemaphoreType.DMA
        any_space = pl.BlockSpec(memory_space=pltpu.HBM)
        bf16, f32 = jnp.bfloat16, jnp.float32
        return pl.pallas_call(
            functools.partial(kernel, nz, nx, near),
            out_shape=jax.ShapeDtypeStruct((rows // 2, out_features), bf16),
            in_specs=[any_space] * 4,
            out_specs=pl.BlockSpec(memory_space=pltpu.VMEM),
            scratch_shapes=[
                pltpu.VMEM((rows, features), bf16),
                pltpu.VMEM((rows, features), bf16),
                pltpu.VMEM((rows, features), bf16),
                pltpu.VMEM((features, out_features), bf16),
                pltpu.VMEM((heads, rows, LANES), bf16),
                pltpu.VMEM((heads, rows // 2, LANES), bf16),
                pltpu.VMEM((2, nz, nx, rows, LANES), bf16),
                pltpu.VMEM((near, rows // 2, LANES), bf16),
                pltpu.VMEM((nq, LANES), bf16),
                pltpu.VMEM((2, nq), f32),
                pltpu.VMEM((HD, nq), f32),
                pltpu.VMEM((nq, LANES), f32),
                pltpu.VMEM((near, rows // 2, LANES), bf16),
                pltpu.VMEM((heads, rows // 2, LANES), bf16),
                pltpu.VMEM((2, rows // 2, features), bf16),
                pltpu.VMEM((rows // 2, out_features), bf16),
                pltpu.VMEM((rows // 2, out_features), bf16),
                dma((nz, 2)), dma((nz,)), dma((nz, 2)), dma((near,)),
                dma((nz, nx)), dma((nz, nx)), dma((nz, nx)), dma((nz, nx)),
                dma((near,)), dma((heads,)), dma, dma, dma((4,)), dma((3,)),
            ],
            compiler_params=pltpu.CompilerParams(
                collective_id=0, has_side_effects=True, vmem_limit_bytes=67043328 - 256 * 1024
            ),
        )(query, key, value, out_weight)

    tokens = P(("grp", "blk", "node"), "pair")
    return jax.shard_map(
        per_device,
        mesh=mesh,
        in_specs=(tokens, tokens, tokens, P("pair", None)),
        out_specs=P(("grp", "blk", "node", "pair"), None),
        check_vma=False,
    )
```
